8 devices in a mesh: dp: 2 (over z, y), dcp: 4 (over x, core).
Axes of the slice: x: 2, y: 2, z: 1, core: 2. Of those that a mesh axis runs over, the one named last changes fastest.
Arguments:
- q_abs: bfloat16 [128, 2, 64, 576], P('dp', None, 'dcp'), parts along dimension 0
- kv_cache: bfloat16 [128, 32, 4, 64, 576], P('dp', None, 'dcp'), parts along dimension 0
- lengths: int32 [128], P('dp'), parts along dimension 0
Outputs:
- output: bfloat16 [128, 2, 64, 512], P('dp', None, 'dcp'), parts along dimension 0
There are 2 independent parts. The reference program is written for one: setup_inputs(seed, part) draws one part's arguments, and reference() takes and returns one part's arrays. A program takes and returns all parts, laid end to end along the dimension named above; each array names one.
All inputs are finite; a program needn't handle non-finite values.
Results may differ from the reference program's by a relative error of at most 0.00787497.
Values are sent between devices in bfloat16 or wider.
A program may use at most 1 GiB of HBM per device.

```python
import math
import jax
import jax.numpy as jnp
from jax import lax

BATCH = 64
MTP = 2
HEADS = 64
LATENT = 512
ROPE = 64
NOPE = 128
ROUNDS = 32
GROUP = 4
PAGE = 64

SEQ = ROUNDS * GROUP * PAGE
WIDTH = LATENT + ROPE


def setup_inputs(seed: int = 0, part: int = 0) -> dict:
    base_key = jax.random.fold_in(jax.random.key(seed), part)
    key_qlat, key_qrope, key_cache, key_len, key_pick = jax.random.split(base_key, 5)
    lat_scale = math.sqrt(SEQ / 256.0)
    q_lat = jax.random.normal(key_qlat, (BATCH, MTP, HEADS, LATENT), jnp.float32) * (math.sqrt(1.8 * (NOPE + ROPE) / LATENT) / lat_scale)
    q_rope = jax.random.normal(key_qrope, (BATCH, MTP, HEADS, ROPE), jnp.float32) * math.sqrt(1.8 * (NOPE + ROPE) / ROPE)
    q_abs = jnp.concatenate([q_lat, q_rope], axis=-1).astype(jnp.bfloat16)
    col_scale = jnp.where(jnp.arange(WIDTH) < LATENT, lat_scale, 1.0)
    kv_cache = (jax.random.normal(key_cache, (BATCH, ROUNDS, GROUP, PAGE, WIDTH), jnp.float32) * col_scale).astype(jnp.bfloat16)
    lengths = jax.random.randint(key_len, (BATCH,), SEQ // 2, SEQ + 1, dtype=jnp.int32)
    longest = jax.random.randint(key_pick, (), 0, BATCH, dtype=jnp.int32)
    lengths = jnp.where(jnp.arange(BATCH) == longest, SEQ, lengths).astype(jnp.int32)
    return {'q_abs': q_abs, 'kv_cache': kv_cache, 'lengths': lengths}


def reference(q_abs, kv_cache, lengths):
    keys_all = kv_cache.reshape(BATCH, SEQ, WIDTH)
    score_scale = (NOPE + ROPE) ** -0.5
    positions = jnp.arange(SEQ)
    offsets = jnp.arange(MTP) - MTP

    def one_seq(seq_args):
        q_seq, key_seq, length = seq_args
        key_f = key_seq.astype(jnp.float32)
        scores = jnp.einsum('thd,sd->ths', q_seq.astype(jnp.float32), key_f) * score_scale
        last_pos = length + offsets
        visible = positions[None, :] <= last_pos[:, None]
        scores = jnp.where(visible[:, None, :], scores, -jnp.inf)
        weights = jax.nn.softmax(scores, axis=-1)
        out_seq = jnp.einsum('ths,sc->thc', weights, key_f[:, :LATENT])
        return out_seq.astype(jnp.bfloat16)

    return lax.map(one_seq, (q_abs, keys_all, lengths))
```

```python
import functools
import math

import jax
import jax.numpy as jnp
from jax import lax
from jax.experimental import pallas as pl
from jax.experimental.pallas import tpu as pltpu
from jax.sharding import PartitionSpec as P

LATENT = 512
ROPE = 64
NOPE = 128
PAGE = 64
MASKED = -1e30
LANES = 128
PAIR = 2
AHEAD = 8
MESH_ID = pl.DeviceIdType.MESH
F32 = jnp.float32
BF16 = jnp.bfloat16


def _nt_dot(a, b):
    return lax.dot_general(a, b, (((1,), (1,)), ((), ())), preferred_element_type=F32)


def _mod2(i):
    return i % 2 if isinstance(i, int) else lax.rem(i, 2)


def _kernel(len_ref, q_hbm, kv_hbm, o_hbm,
            q_own, q_lat, q_rope, kv_buf, s_a, s_b, p_a, p_b,
            keep, part_send, part_recv, mine, mine_lse,
            ici_send, ici_recv, lse_send, lse_recv, out_buf,
            own_sem, kv_sem, qs_sem, qr_sem, part_ssem, part_rsem, ici_ssem, ici_rsem, out_sem):
    batch, toks, heads, width = q_own.shape
    steps = batch // PAIR
    seq_loc = kv_buf.shape[2]
    rows = toks * heads
    tile = LANES
    group = 4
    me = lax.axis_index('dcp')
    core = lax.rem(me, 2)
    partner = me + 1 - 2 * core
    across = lax.rem(me + 2, group)

    barrier = pltpu.get_barrier_semaphore()
    for peer in (partner, across):
        pl.semaphore_signal(barrier, inc=1, device_id={'dcp': peer}, device_id_type=MESH_ID)

    own_copy = pltpu.make_async_copy(q_hbm, q_own, own_sem.at[0])
    own_copy.start()

    def kv_copy(i, s):
        slot = _mod2(i)
        return pltpu.make_async_copy(kv_hbm.at[PAIR * i + s], kv_buf.at[slot, s], kv_sem.at[slot, s])

    for s in range(PAIR):
        kv_copy(0, s).start()

    def pair(i):
        return pl.ds(PAIR * i, PAIR)

    def q_send(i, dest):
        slot = (2, 1, 3)[dest]
        peer = (partner, across, partner)[dest]
        if dest == 2:
            lat_src, rope_src = q_lat.at[pair(i), 1], q_rope.at[pair(i), 1]
        else:
            lat_src, rope_src = q_own.at[pair(i), :, :, pl.ds(0, LATENT)], q_rope.at[pair(i), 0]
        lat = pltpu.make_async_remote_copy(
            src_ref=lat_src, dst_ref=q_lat.at[pair(i), slot],
            send_sem=qs_sem.at[dest, 0, i], recv_sem=qr_sem.at[slot - 1, 0, i],
            device_id={'dcp': peer}, device_id_type=MESH_ID)
        rope = pltpu.make_async_remote_copy(
            src_ref=rope_src, dst_ref=q_rope.at[pair(i), slot],
            send_sem=qs_sem.at[dest, 1, i], recv_sem=qr_sem.at[slot - 1, 1, i],
            device_id={'dcp': peer}, device_id_type=MESH_ID)
        return lat, rope

    def q_start(i, dest):
        for c in q_send(i, dest):
            c.start()

    def q_arrived(i, dest):
        for c in q_send(i, dest):
            c.wait_recv()

    def part_copy(i):
        slot = _mod2(i)
        return pltpu.make_async_remote_copy(
            src_ref=part_send.at[slot], dst_ref=part_recv.at[i],
            send_sem=part_ssem.at[slot], recv_sem=part_rsem.at[i],
            device_id={'dcp': partner}, device_id_type=MESH_ID)

    def ici_copies(i):
        out = pltpu.make_async_remote_copy(
            src_ref=ici_send.at[i], dst_ref=ici_recv.at[i],
            send_sem=ici_ssem.at[0, i], recv_sem=ici_rsem.at[0, i],
            device_id={'dcp': across}, device_id_type=MESH_ID)
        lse = pltpu.make_async_remote_copy(
            src_ref=lse_send.at[i], dst_ref=lse_recv.at[i],
            send_sem=ici_ssem.at[1, i], recv_sem=ici_rsem.at[1, i],
            device_id={'dcp': across}, device_id_type=MESH_ID)
        return out, lse

    def out_copy(i):
        return pltpu.make_async_copy(out_buf.at[pair(i)], o_hbm.at[pair(i)], out_sem.at[i])

    own_copy.wait()

    def pack(b, carry):
        first = q_own[b, 0, :, LATENT:width]
        second = q_own[b, 1, :, LATENT:width]
        q_rope[b, 0] = jnp.concatenate([first, second], axis=-1)
        return carry

    lax.fori_loop(0, batch, pack, 0)
    pl.semaphore_wait(barrier, 2)
    for i in range(AHEAD):
        q_start(i, 1)
        q_start(i, 0)

    scale2 = (NOPE + ROPE) ** -0.5 * math.log2(math.e)
    row_tok = lax.rem(lax.broadcasted_iota(jnp.int32, (group * rows, 1), 0) // heads, toks)
    col = lax.broadcasted_iota(jnp.int32, (1, seq_loc), 1)
    col_pos = (col // PAGE) * (group * PAGE) + lax.rem(col, PAGE) + me * PAGE
    half = lax.broadcasted_iota(jnp.int32, (group * rows // 2, LANES), 1) < LANES // 2

    def load_q(b):
        own = q_own[b, :, :, 0:LATENT].reshape(rows, LATENT)
        others = q_lat[b, 1:4].reshape(3 * rows, LATENT)
        lat = jnp.concatenate([own, others], axis=0)
        packed = q_rope[b]
        first = packed[:, :, 0:ROPE]
        second = packed[:, :, ROPE:2 * ROPE]
        rope = jnp.stack([first, second], axis=1).reshape(group * rows, ROPE)
        return lat, rope

    def scores(i, s, s_ref):
        slot = _mod2(i)
        b = PAIR * i + s
        lat, rope = load_q(b)
        last = len_ref[b] - toks + row_tok
        best = None
        chunk = 512
        for n in range(seq_loc // chunk):
            at = pl.ds(n * chunk, chunk)
            sc = _nt_dot(lat, kv_buf[slot, s, at, 0:LATENT]) + _nt_dot(rope, kv_buf[slot, s, at, LATENT:width])
            sc = jnp.where(col_pos[:, n * chunk:(n + 1) * chunk] <= last, sc * scale2, MASKED)
            s_ref[:, at] = sc
            for t in range(chunk // tile):
                piece = sc[:, t * tile:(t + 1) * tile]
                best = piece if best is None else jnp.maximum(best, piece)
        return jnp.max(best, axis=1, keepdims=True)

    def attend(i, s, s_ref, p_ref, top):
        slot = _mod2(i)
        total = None
        for n in range(seq_loc // tile):
            w = jnp.exp2(s_ref[:, n * tile:(n + 1) * tile] - top)
            total = w if total is None else total + w
            p_ref[:, n * tile:(n + 1) * tile] = w.astype(BF16)
        out = jnp.dot(p_ref[...], kv_buf[slot, s, :, 0:LATENT], preferred_element_type=F32)
        norm = jnp.sum(total, axis=1, keepdims=True)
        stats = jnp.where(half[0:1], top, norm)
        h = group * rows // 2
        keep[slot, s, :, 0:LATENT] = out[:h]
        keep[slot, s, :, LATENT:LATENT + LANES] = stats[:h]
        part_send[slot, s, :, 0:LATENT] = out[h:]
        part_send[slot, s, :, LATENT:LATENT + LANES] = stats[h:]

    row_id = lax.broadcasted_iota(jnp.int32, (rows, LANES), 0)
    lane_id = lax.broadcasted_iota(jnp.int32, (rows, LANES), 1)

    def merge(i):
        slot = _mod2(i)
        lse_row = None
        for s in range(PAIR):
            st_a = keep[slot, s, :, LATENT:LATENT + LANES]
            st_b = part_recv[i, s, :, LATENT:LATENT + LANES]
            m_a, l_a = st_a[:, 0:1], st_a[:, LANES // 2:LANES // 2 + 1]
            m_b, l_b = st_b[:, 0:1], st_b[:, LANES // 2:LANES // 2 + 1]
            m = jnp.maximum(m_a, m_b)
            w_a, w_b = jnp.exp2(m_a - m), jnp.exp2(m_b - m)
            norm = l_a * w_a + l_b * w_b
            lse = m + jnp.log2(norm)
            inv = 1.0 / norm
            both = keep[slot, s, :, 0:LATENT] * (w_a * inv) + part_recv[i, s, :, 0:LATENT] * (w_b * inv)
            mine[i, s] = both[:rows]
            ici_send[i, s] = both[rows:].astype(BF16)
            wide = jnp.broadcast_to(lse, (2 * rows, LANES))
            mine_lse[i, s] = wide[:rows]
            picked = jnp.where(lane_id == row_id + s * rows, wide[rows:], 0.0)
            lse_row = picked if lse_row is None else lse_row + picked
        lse_send[i] = jnp.sum(lse_row, axis=0, keepdims=True)

    def finish(i):
        row = jnp.broadcast_to(lse_recv[i], (rows, LANES))
        for s in range(PAIR):
            lse_b = jnp.sum(jnp.where(lane_id == row_id + s * rows, row, 0.0), axis=1, keepdims=True)
            lse_a = mine_lse[i, s, :, 0:1]
            m = jnp.maximum(lse_a, lse_b)
            w_a, w_b = jnp.exp2(lse_a - m), jnp.exp2(lse_b - m)
            inv = 1.0 / (w_a + w_b)
            o = mine[i, s] * (w_a * inv) + ici_recv[i, s].astype(F32) * (w_b * inv)
            out_buf[PAIR * i + s] = o.astype(BF16).reshape(toks, heads, LATENT)

    def step(i, compute, merging, sending, first=False):
        if sending:
            for c in ici_copies(i - 3):
                c.start()
        if merging:
            part_copy(i - 2).wait()
        if compute or merging:
            if not first:
                if isinstance(i, int) and i - 1 >= steps:
                    pass
                else:
                    part_copy(i - 1).start()
        if compute:
            for s in range(PAIR):
                kv_copy(i, s).wait()

            def prefetch():
                for s in range(PAIR):
                    kv_copy(i + 1, s).start()
                q_arrived(i + 1, 1)
                q_start(i + 1, 2)

            def more():
                q_start(i + AHEAD, 1)
                q_start(i + AHEAD, 0)

            if isinstance(i, int):
                if i + 1 < steps:
                    prefetch()
                if i + AHEAD < steps:
                    more()
            else:
                pl.when(i + AHEAD < steps)(more)
                pl.when(i + 1 < steps)(prefetch)
            q_arrived(i, 0)
            q_arrived(i, 2)
        if merging:
            merge(i - 2)
        if compute:
            tops = [scores(i, 0, s_a), scores(i, 1, s_b)]
            attend(i, 0, s_a, p_a, tops[0])
            attend(i, 1, s_b, p_b, tops[1])

    q_arrived(0, 1)
    q_start(0, 2)
    step(0, True, False, False, first=True)
    step(1, True, False, False)
    step(2, True, True, False)

    def body(i, carry):
        step(i, True, True, True)
        return carry

    lax.fori_loop(3, steps, body, 0)
    step(steps, False, True, True)
    step(steps + 1, False, True, True)
    step(steps + 2, False, False, True)

    def tail(i, carry):
        for c in ici_copies(i):
            c.wait_recv()
        finish(i)
        out_copy(i).start()
        return carry

    lax.fori_loop(0, steps, tail, 0)

    def drain(i, carry):
        out_copy(i).wait()
        for c in ici_copies(i):
            c.wait_send()
        for dest in range(3):
            for c in q_send(i, dest):
                c.wait_send()
        return carry

    lax.fori_loop(0, steps, drain, 0)


def solution(mesh):
    def local_step(q_blk, kv_blk, len_blk):
        batch, toks, heads, width = q_blk.shape
        rounds = kv_blk.shape[1]
        seq_loc = rounds * PAGE
        steps = batch // PAIR
        rows = toks * heads
        keys = kv_blk.reshape(batch, seq_loc, width)
        wide = LATENT + LANES
        dma = pltpu.SemaphoreType.DMA
        return pl.pallas_call(
            _kernel,
            out_shape=jax.ShapeDtypeStruct((batch, toks, heads, LATENT), BF16),
            in_specs=[
                pl.BlockSpec(memory_space=pltpu.SMEM),
                pl.BlockSpec(memory_space=pl.ANY),
                pl.BlockSpec(memory_space=pl.ANY),
            ],
            out_specs=pl.BlockSpec(memory_space=pl.ANY),
            scratch_shapes=[
                pltpu.VMEM((batch, toks, heads, width), BF16),
                pltpu.VMEM((batch, 4, toks, heads, LATENT), BF16),
                pltpu.VMEM((batch, 4, heads, toks * ROPE), BF16),
                pltpu.VMEM((2, PAIR, seq_loc, width), BF16),
                pltpu.VMEM((4 * rows, seq_loc), F32),
                pltpu.VMEM((4 * rows, seq_loc), F32),
                pltpu.VMEM((4 * rows, seq_loc), BF16),
                pltpu.VMEM((4 * rows, seq_loc), BF16),
                pltpu.VMEM((2, PAIR, 2 * rows, wide), F32),
                pltpu.VMEM((2, PAIR, 2 * rows, wide), F32),
                pltpu.VMEM((steps, PAIR, 2 * rows, wide), F32),
                pltpu.VMEM((steps, PAIR, rows, LATENT), F32),
                pltpu.VMEM((steps, PAIR, rows, LANES), F32),
                pltpu.VMEM((steps, PAIR, rows, LATENT), BF16),
                pltpu.VMEM((steps, PAIR, rows, LATENT), BF16),
                pltpu.VMEM((steps, 1, LANES), F32),
                pltpu.VMEM((steps, 1, LANES), F32),
                pltpu.VMEM((batch, toks, heads, LATENT), BF16),
                dma((1,)),
                dma((2, PAIR)),
                dma((3, 2, steps)),
                dma((3, 2, steps)),
                dma((2,)),
                dma((steps,)),
                dma((2, steps)),
                dma((2, steps)),
                dma((steps,)),
            ],
            compiler_params=pltpu.CompilerParams(
                collective_id=0, has_side_effects=True, vmem_limit_bytes=66_000_000),
            name='mla_decode',
        )(len_blk, q_blk, keys)

    return jax.shard_map(
        local_step, mesh=mesh,
        in_specs=(P('dp', None, 'dcp', None), P('dp', None, 'dcp', None, None), P('dp')),
        out_specs=P('dp', None, 'dcp', None), check_vma=False)
```

```python
import functools
import math

import jax
import jax.numpy as jnp
from jax import lax
from jax.experimental import pallas as pl
from jax.experimental.pallas import tpu as pltpu
from jax.sharding import PartitionSpec as P

LATENT = 512
ROPE = 64
NOPE = 128
PAGE = 64
MASKED = -1e30
LANES = 128
PAIR = 2
AHEAD = 8
DEPTH = 3
MESH_ID = pl.DeviceIdType.MESH
F32 = jnp.float32
BF16 = jnp.bfloat16


def _nt_dot(a, b):
    return lax.dot_general(a, b, (((1,), (1,)), ((), ())), preferred_element_type=F32)


def _mod(i, n):
    return i % n if isinstance(i, int) else lax.rem(i, n)


def _kernel(len_ref, q_hbm, kv_hbm, out_buf,
            q_own, q_lat, q_rope, kv_buf, s_a, s_b, p_a, p_b,
            keep, part_send, part_recv, mine, mine_lse,
            ici_send, ici_recv, lse_send, lse_recv,
            own_sem, kv_sem, qs_sem, qr_sem, part_ssem, part_rsem, ici_ssem, ici_rsem):
    batch, toks, heads, width = q_own.shape
    steps = batch // PAIR
    seq_loc = kv_buf.shape[2]
    rows = toks * heads
    tile = LANES
    group = 4
    me = lax.axis_index('dcp')
    core = lax.rem(me, 2)
    partner = me + 1 - 2 * core
    across = lax.rem(me + 2, group)

    barrier = pltpu.get_barrier_semaphore()
    for peer in (partner, across):
        pl.semaphore_signal(barrier, inc=1, device_id={'dcp': peer}, device_id_type=MESH_ID)

    early = PAIR * AHEAD
    own_copies = []
    for k, (lo, n) in enumerate(((0, early), (early, batch - early))):
        own_copies.append(pltpu.make_async_copy(q_hbm.at[pl.ds(lo, n)], q_own.at[pl.ds(lo, n)], own_sem.at[k]))
        own_copies[-1].start()

    def kv_copy(i, s):
        slot = _mod(i, DEPTH)
        return pltpu.make_async_copy(kv_hbm.at[PAIR * i + s], kv_buf.at[slot, s], kv_sem.at[slot, s])

    for i in range(DEPTH - 1):
        for s in range(PAIR):
            kv_copy(i, s).start()

    def pair(i):
        return pl.ds(PAIR * i, PAIR)

    def q_send(i, dest):
        slot = (2, 1, 3)[dest]
        peer = (partner, across, partner)[dest]
        if dest == 2:
            lat_src, rope_src = q_lat.at[pair(i), 1], q_rope.at[pair(i), 1]
        else:
            lat_src, rope_src = q_own.at[pair(i), :, :, pl.ds(0, LATENT)], q_rope.at[pair(i), 0]
        lat = pltpu.make_async_remote_copy(
            src_ref=lat_src, dst_ref=q_lat.at[pair(i), slot],
            send_sem=qs_sem.at[dest, 0, i], recv_sem=qr_sem.at[slot - 1, 0, i],
            device_id={'dcp': peer}, device_id_type=MESH_ID)
        rope = pltpu.make_async_remote_copy(
            src_ref=rope_src, dst_ref=q_rope.at[pair(i), slot],
            send_sem=qs_sem.at[dest, 1, i], recv_sem=qr_sem.at[slot - 1, 1, i],
            device_id={'dcp': peer}, device_id_type=MESH_ID)
        return lat, rope

    def q_start(i, dest):
        for c in q_send(i, dest):
            c.start()

    def q_arrived(i, dest):
        for c in q_send(i, dest):
            c.wait_recv()

    def part_copy(i):
        slot = _mod(i, 2)
        return pltpu.make_async_remote_copy(
            src_ref=part_send.at[slot], dst_ref=part_recv.at[i],
            send_sem=part_ssem.at[slot], recv_sem=part_rsem.at[i],
            device_id={'dcp': partner}, device_id_type=MESH_ID)

    def ici_copies(i):
        out = pltpu.make_async_remote_copy(
            src_ref=ici_send.at[i], dst_ref=ici_recv.at[i],
            send_sem=ici_ssem.at[0, i], recv_sem=ici_rsem.at[0, i],
            device_id={'dcp': across}, device_id_type=MESH_ID)
        lse = pltpu.make_async_remote_copy(
            src_ref=lse_send.at[i], dst_ref=lse_recv.at[i],
            send_sem=ici_ssem.at[1, i], recv_sem=ici_rsem.at[1, i],
            device_id={'dcp': across}, device_id_type=MESH_ID)
        return out, lse

    unroll = 8

    def pack(k, carry):
        for u in range(unroll):
            b = unroll * k + u
            first = q_own[b, 0, :, LATENT:width]
            second = q_own[b, 1, :, LATENT:width]
            q_rope[b, 0] = jnp.concatenate([first, second], axis=-1)
        return carry

    own_copies[0].wait()
    lax.fori_loop(0, early // unroll, pack, 0)
    pl.semaphore_wait(barrier, 2)
    for i in range(AHEAD):
        q_start(i, 1)
        q_start(i, 0)
    own_copies[1].wait()
    lax.fori_loop(early // unroll, batch // unroll, pack, 0)

    scale2 = (NOPE + ROPE) ** -0.5 * math.log2(math.e)
    row_tok = lax.rem(lax.broadcasted_iota(jnp.int32, (group * rows, 1), 0) // heads, toks)
    col = lax.broadcasted_iota(jnp.int32, (1, seq_loc), 1)
    col_pos = (col // PAGE) * (group * PAGE) + lax.rem(col, PAGE) + me * PAGE
    half = lax.broadcasted_iota(jnp.int32, (group * rows // 2, LANES), 1) < LANES // 2

    def load_q(b):
        own = q_own[b, :, :, 0:LATENT].reshape(rows, LATENT)
        others = q_lat[b, 1:4].reshape(3 * rows, LATENT)
        lat = jnp.concatenate([own, others], axis=0)
        packed = q_rope[b]
        first = packed[:, :, 0:ROPE]
        second = packed[:, :, ROPE:2 * ROPE]
        rope = jnp.stack([first, second], axis=1).reshape(group * rows, ROPE)
        return lat, rope

    def scores(i, s, s_ref):
        slot = _mod(i, DEPTH)
        b = PAIR * i + s
        lat, rope = load_q(b)
        last = len_ref[b] - toks + row_tok
        best = None
        chunk = 512
        for n in range(seq_loc // chunk):
            at = pl.ds(n * chunk, chunk)
            sc = _nt_dot(lat, kv_buf[slot, s, at, 0:LATENT]) + _nt_dot(rope, kv_buf[slot, s, at, LATENT:width])
            sc = jnp.where(col_pos[:, n * chunk:(n + 1) * chunk] <= last, sc * scale2, MASKED)
            s_ref[:, at] = sc
            for t in range(chunk // tile):
                piece = sc[:, t * tile:(t + 1) * tile]
                best = piece if best is None else jnp.maximum(best, piece)
        return jnp.max(best, axis=1, keepdims=True)

    def attend(i, s, s_ref, p_ref, top):
        slot, held = _mod(i, 2), _mod(i, DEPTH)
        total = None
        for n in range(seq_loc // tile):
            w = jnp.exp2(s_ref[:, n * tile:(n + 1) * tile] - top)
            total = w if total is None else total + w
            p_ref[:, n * tile:(n + 1) * tile] = w.astype(BF16)
        out = jnp.dot(p_ref[...], kv_buf[held, s, :, 0:LATENT], preferred_element_type=F32)
        norm = jnp.sum(total, axis=1, keepdims=True)
        stats = jnp.where(half[0:1], top, norm)
        h = group * rows // 2
        keep[slot, s, :, 0:LATENT] = out[:h]
        keep[slot, s, :, LATENT:LATENT + LANES] = stats[:h]
        part_send[slot, s, :, 0:LATENT] = out[h:]
        part_send[slot, s, :, LATENT:LATENT + LANES] = stats[h:]

    row_id = lax.broadcasted_iota(jnp.int32, (rows, LANES), 0)
    lane_id = lax.broadcasted_iota(jnp.int32, (rows, LANES), 1)

    def merge(i):
        slot = _mod(i, 2)
        lse_row = None
        for s in range(PAIR):
            st_a = keep[slot, s, :, LATENT:LATENT + LANES]
            st_b = part_recv[i, s, :, LATENT:LATENT + LANES]
            m_a, l_a = st_a[:, 0:1], st_a[:, LANES // 2:LANES // 2 + 1]
            m_b, l_b = st_b[:, 0:1], st_b[:, LANES // 2:LANES // 2 + 1]
            m = jnp.maximum(m_a, m_b)
            w_a, w_b = jnp.exp2(m_a - m), jnp.exp2(m_b - m)
            norm = l_a * w_a + l_b * w_b
            lse = m + jnp.log2(norm)
            inv = 1.0 / norm
            both = keep[slot, s, :, 0:LATENT] * (w_a * inv) + part_recv[i, s, :, 0:LATENT] * (w_b * inv)
            mine[i, s] = both[:rows]
            ici_send[i, s] = both[rows:].astype(BF16)
            wide = jnp.broadcast_to(lse, (2 * rows, LANES))
            mine_lse[i, s] = wide[:rows]
            picked = jnp.where(lane_id == row_id + s * rows, wide[rows:], 0.0)
            lse_row = picked if lse_row is None else lse_row + picked
        lse_send[i] = jnp.sum(lse_row, axis=0, keepdims=True)

    def finish(i):
        row = jnp.broadcast_to(lse_recv[i], (rows, LANES))
        for s in range(PAIR):
            lse_b = jnp.sum(jnp.where(lane_id == row_id + s * rows, row, 0.0), axis=1, keepdims=True)
            lse_a = mine_lse[i, s, :, 0:1]
            m = jnp.maximum(lse_a, lse_b)
            w_a, w_b = jnp.exp2(lse_a - m), jnp.exp2(lse_b - m)
            inv = 1.0 / (w_a + w_b)
            o = mine[i, s] * (w_a * inv) + ici_recv[i, s].astype(F32) * (w_b * inv)
            out_buf[PAIR * i + s] = o.astype(BF16).reshape(toks, heads, LATENT)

    def step(i, compute, merging, sending, first=False):
        if sending:
            for c in ici_copies(i - 3):
                c.start()
        if merging:
            part_copy(i - 2).wait()
        if compute or merging:
            if not first:
                if isinstance(i, int) and i - 1 >= steps:
                    pass
                else:
                    part_copy(i - 1).start()
        if compute:
            for s in range(PAIR):
                kv_copy(i, s).wait()

            def prefetch():
                for s in range(PAIR):
                    kv_copy(i + DEPTH - 1, s).start()

            def forward():
                q_arrived(i + 1, 1)
                q_start(i + 1, 2)

            def more():
                q_start(i + AHEAD, 1)
                q_start(i + AHEAD, 0)

            if isinstance(i, int):
                if i + DEPTH - 1 < steps:
                    prefetch()
                if i + AHEAD < steps:
                    more()
                if i + 1 < steps:
                    forward()
            else:
                pl.when(i + DEPTH - 1 < steps)(prefetch)
                pl.when(i + AHEAD < steps)(more)
                pl.when(i + 1 < steps)(forward)
            q_arrived(i, 0)
            q_arrived(i, 2)
        if merging:
            merge(i - 2)
        if compute:
            tops = [scores(i, 0, s_a), scores(i, 1, s_b)]
            attend(i, 0, s_a, p_a, tops[0])
            attend(i, 1, s_b, p_b, tops[1])

    q_arrived(0, 1)
    q_start(0, 2)
    step(0, True, False, False, first=True)
    step(1, True, False, False)
    step(2, True, True, False)

    def body(i, carry):
        step(i, True, True, True)
        return carry

    lax.fori_loop(3, steps, body, 0)
    step(steps, False, True, True)
    step(steps + 1, False, True, True)
    step(steps + 2, False, False, True)

    def arrive(i):
        for dest in range(3):
            for c in q_send(i, dest):
                c.wait_send()
        for c in ici_copies(i):
            c.wait()

    def tail(k, carry):
        for u in range(4):
            arrive(4 * k + u)
        for u in range(4):
            finish(4 * k + u)
        return carry

    lax.fori_loop(0, steps // 4 - 1, tail, 0)
    for i in range(steps - 4, steps):
        arrive(i)
        finish(i)


def solution(mesh):
    def local_step(q_blk, kv_blk, len_blk):
        batch, toks, heads, width = q_blk.shape
        rounds = kv_blk.shape[1]
        seq_loc = rounds * PAGE
        steps = batch // PAIR
        rows = toks * heads
        keys = kv_blk.reshape(batch, seq_loc, width)
        wide = LATENT + LANES
        dma = pltpu.SemaphoreType.DMA
        return pl.pallas_call(
            _kernel,
            out_shape=pltpu.VMEM((batch, toks, heads, LATENT), BF16),
            in_specs=[
                pl.BlockSpec(memory_space=pltpu.SMEM),
                pl.BlockSpec(memory_space=pl.ANY),
                pl.BlockSpec(memory_space=pl.ANY),
            ],
            out_specs=pl.BlockSpec(memory_space=pltpu.VMEM),
            scratch_shapes=[
                pltpu.VMEM((batch, toks, heads, width), BF16),
                pltpu.VMEM((batch, 4, toks, heads, LATENT), BF16),
                pltpu.VMEM((batch, 4, heads, toks * ROPE), BF16),
                pltpu.VMEM((DEPTH, PAIR, seq_loc, width), BF16),
                pltpu.VMEM((4 * rows, seq_loc), F32),
                pltpu.VMEM((4 * rows, seq_loc), F32),
                pltpu.VMEM((4 * rows, seq_loc), BF16),
                pltpu.VMEM((4 * rows, seq_loc), BF16),
                pltpu.VMEM((2, PAIR, 2 * rows, wide), F32),
                pltpu.VMEM((2, PAIR, 2 * rows, wide), F32),
                pltpu.VMEM((steps, PAIR, 2 * rows, wide), F32),
                pltpu.VMEM((steps, PAIR, rows, LATENT), F32),
                pltpu.VMEM((steps, PAIR, rows, LANES), F32),
                pltpu.VMEM((steps, PAIR, rows, LATENT), BF16),
                pltpu.VMEM((steps, PAIR, rows, LATENT), BF16),
                pltpu.VMEM((steps, 1, LANES), F32),
                pltpu.VMEM((steps, 1, LANES), F32),
                dma((2,)),
                dma((DEPTH, PAIR)),
                dma((3, 2, steps)),
                dma((3, 2, steps)),
                dma((2,)),
                dma((steps,)),
                dma((2, steps)),
                dma((2, steps)),
            ],
            compiler_params=pltpu.CompilerParams(
                collective_id=0, has_side_effects=True, vmem_limit_bytes=60_000_000),
            name='mla_decode',
        )(len_blk, q_blk, keys)

    return jax.shard_map(
        local_step, mesh=mesh,
        in_specs=(P('dp', None, 'dcp', None), P('dp', None, 'dcp', None, None), P('dp')),
        out_specs=P('dp', None, 'dcp', None), check_vma=False)
```

```python
import functools
import math

import jax
import jax.numpy as jnp
from jax import lax
from jax.experimental import pallas as pl
from jax.experimental.pallas import tpu as pltpu
from jax.sharding import PartitionSpec as P

LATENT = 512
ROPE = 64
NOPE = 128
PAGE = 64
MASKED = -1e30
LANES = 128
PAIR = 2
FIRST = 2
AHEAD = 8
LSE_STEPS = 4
DEPTH = 3
MESH_ID = pl.DeviceIdType.MESH
F32 = jnp.float32
BF16 = jnp.bfloat16


def _nt_dot(a, b):
    return lax.dot_general(a, b, (((1,), (1,)), ((), ())), preferred_element_type=F32)


def _mod(i, n):
    return i % n if isinstance(i, int) else lax.rem(i, n)


def _kernel(len_ref, q_hbm, kv_hbm, out_buf,
            q_own, q_msg, kv_buf, s_a, s_b, p_a, p_b,
            keep, part_send, part_recv, mine, mine_lse,
            ici_send, ici_recv, lse_send, lse_recv,
            own_sem, kv_sem, qs_sem, qr_sem, part_ssem, part_rsem, ici_ssem, ici_rsem):
    batch, toks, heads, width = q_own.shape
    steps = batch // PAIR
    seq_loc = kv_buf.shape[2]
    rows = toks * heads
    tile = LANES
    group = 4
    me = lax.axis_index('dcp')
    core = lax.rem(me, 2)
    partner = me + 1 - 2 * core
    across = lax.rem(me + 2, group)

    barrier = pltpu.get_barrier_semaphore()
    for peer in (partner, across):
        pl.semaphore_signal(barrier, inc=1, device_id={'dcp': peer}, device_id_type=MESH_ID)

    cuts = (0, PAIR * FIRST, PAIR * AHEAD, batch)
    own_copies = []
    for k in range(3):
        at = pl.ds(cuts[k], cuts[k + 1] - cuts[k])
        own_copies.append(pltpu.make_async_copy(q_hbm.at[at], q_own.at[at], own_sem.at[k]))
        own_copies[-1].start()

    def kv_copy(i, s):
        slot = _mod(i, DEPTH)
        return pltpu.make_async_copy(kv_hbm.at[PAIR * i + s], kv_buf.at[slot, s], kv_sem.at[slot, s])

    def pair(i):
        return pl.ds(PAIR * i, PAIR)

    def q_send(i, dest):
        slot = (2, 1, 3)[dest]
        return pltpu.make_async_remote_copy(
            src_ref=q_msg.at[1 if dest == 2 else 0, pair(i)], dst_ref=q_msg.at[slot, pair(i)],
            send_sem=qs_sem.at[dest, i], recv_sem=qr_sem.at[slot - 1, i],
            device_id={'dcp': (partner, across, partner)[dest]}, device_id_type=MESH_ID)

    def part_copy(i):
        slot = _mod(i, 2)
        return pltpu.make_async_remote_copy(
            src_ref=part_send.at[slot], dst_ref=part_recv.at[i],
            send_sem=part_ssem.at[slot], recv_sem=part_rsem.at[i],
            device_id={'dcp': partner}, device_id_type=MESH_ID)

    def out_send(i):
        return pltpu.make_async_remote_copy(
            src_ref=ici_send.at[i], dst_ref=ici_recv.at[i],
            send_sem=ici_ssem.at[0, i], recv_sem=ici_rsem.at[0, i],
            device_id={'dcp': across}, device_id_type=MESH_ID)

    def lse_row(i):
        if isinstance(i, int) and i == steps - 1:
            return steps // LSE_STEPS, 0
        return i // LSE_STEPS, _mod(i, LSE_STEPS)

    def lse_send_copy(k):
        return pltpu.make_async_remote_copy(
            src_ref=lse_send.at[k], dst_ref=lse_recv.at[k],
            send_sem=ici_ssem.at[1, k], recv_sem=ici_rsem.at[1, k],
            device_id={'dcp': across}, device_id_type=MESH_ID)

    unroll = PAIR * FIRST
    lat_tiles = LATENT // LANES

    def pack(k, carry):
        for u in range(unroll):
            b = unroll * k + u
            for t in range(toks):
                for n in range(lat_tiles):
                    q_msg[0, b, t * lat_tiles + n] = q_own[b, t, :, n * LANES:(n + 1) * LANES]
            q_msg[0, b, toks * lat_tiles] = jnp.concatenate(
                [q_own[b, t, :, LATENT:width] for t in range(toks)], axis=-1)
        return carry

    own_copies[0].wait()
    pack(0, 0)
    pl.semaphore_wait(barrier, 2)
    for k in range(2):
        if k == 1:
            own_copies[1].wait()
            lax.fori_loop(1, cuts[2] // unroll, pack, 0)
        for i in range(cuts[k] // PAIR, cuts[k + 1] // PAIR):
            q_send(i, 1).start()
            q_send(i, 0).start()
    for i in range(DEPTH - 1):
        for s in range(PAIR):
            kv_copy(i, s).start()
    own_copies[2].wait()
    lax.fori_loop(cuts[2] // unroll, batch // unroll, pack, 0)

    scale2 = (NOPE + ROPE) ** -0.5 * math.log2(math.e)
    row_tok = lax.rem(lax.broadcasted_iota(jnp.int32, (group * rows, 1), 0) // heads, toks)
    col = lax.broadcasted_iota(jnp.int32, (1, seq_loc), 1)
    col_pos = (col // PAGE) * (group * PAGE) + lax.rem(col, PAGE) + me * PAGE
    half = lax.broadcasted_iota(jnp.int32, (group * rows // 2, LANES), 1) < LANES // 2

    def load_q(b):
        lat = jnp.concatenate(
            [jnp.concatenate([q_msg[g, b, t * lat_tiles + n] for n in range(lat_tiles)], axis=1)
             for g in range(group) for t in range(toks)], axis=0)
        rope = jnp.concatenate(
            [q_msg[g, b, toks * lat_tiles][:, t * ROPE:(t + 1) * ROPE]
             for g in range(group) for t in range(toks)], axis=0)
        return lat, rope

    def scores(i, s, s_ref):
        slot = _mod(i, DEPTH)
        b = PAIR * i + s
        lat, rope = load_q(b)
        last = len_ref[b] - toks + row_tok
        best = None
        chunk = 512
        for n in range(seq_loc // chunk):
            at = pl.ds(n * chunk, chunk)
            sc = _nt_dot(lat, kv_buf[slot, s, at, 0:LATENT]) + _nt_dot(rope, kv_buf[slot, s, at, LATENT:width])
            sc = jnp.where(col_pos[:, n * chunk:(n + 1) * chunk] <= last, sc * scale2, MASKED)
            s_ref[:, at] = sc
            for t in range(chunk // tile):
                piece = sc[:, t * tile:(t + 1) * tile]
                best = piece if best is None else jnp.maximum(best, piece)
        return jnp.max(best, axis=1, keepdims=True)

    def attend(i, s, s_ref, p_ref, top):
        slot, held = _mod(i, 2), _mod(i, DEPTH)
        total = None
        for n in range(seq_loc // tile):
            w = jnp.exp2(s_ref[:, n * tile:(n + 1) * tile] - top)
            total = w if total is None else total + w
            p_ref[:, n * tile:(n + 1) * tile] = w.astype(BF16)
        out = jnp.dot(p_ref[...], kv_buf[held, s, :, 0:LATENT], preferred_element_type=F32)
        norm = jnp.sum(total, axis=1, keepdims=True)
        stats = jnp.where(half[0:1], top, norm)
        h = group * rows // 2
        keep[slot, s, :, 0:LATENT] = out[:h]
        keep[slot, s, :, LATENT:LATENT + LANES] = stats[:h]
        part_send[slot, s, :, 0:LATENT] = out[h:]
        part_send[slot, s, :, LATENT:LATENT + LANES] = stats[h:]

    row_id = lax.broadcasted_iota(jnp.int32, (rows, LANES), 0)
    lane_id = lax.broadcasted_iota(jnp.int32, (rows, LANES), 1)

    def merge(i):
        slot = _mod(i, 2)
        lse_sum = None
        for s in range(PAIR):
            st_a = keep[slot, s, :, LATENT:LATENT + LANES]
            st_b = part_recv[i, s, :, LATENT:LATENT + LANES]
            m_a, l_a = st_a[:, 0:1], st_a[:, LANES // 2:LANES // 2 + 1]
            m_b, l_b = st_b[:, 0:1], st_b[:, LANES // 2:LANES // 2 + 1]
            m = jnp.maximum(m_a, m_b)
            w_a, w_b = jnp.exp2(m_a - m), jnp.exp2(m_b - m)
            norm = l_a * w_a + l_b * w_b
            lse = m + jnp.log2(norm)
            inv = 1.0 / norm
            both = keep[slot, s, :, 0:LATENT] * (w_a * inv) + part_recv[i, s, :, 0:LATENT] * (w_b * inv)
            mine[i, s] = both[:rows]
            ici_send[i, s] = both[rows:].astype(BF16)
            wide = jnp.broadcast_to(lse, (2 * rows, LANES))
            mine_lse[i, s] = wide[:rows]
            picked = jnp.where(lane_id == row_id + s * rows, wide[rows:], 0.0)
            lse_sum = picked if lse_sum is None else lse_sum + picked
        k, r = lse_row(i)
        lse_send[k, pl.ds(r, 1)] = jnp.sum(lse_sum, axis=0, keepdims=True)

    def finish(i):
        k, r = lse_row(i)
        row = jnp.broadcast_to(lse_recv[k, pl.ds(r, 1)], (rows, LANES))
        for s in range(PAIR):
            lse_b = jnp.sum(jnp.where(lane_id == row_id + s * rows, row, 0.0), axis=1, keepdims=True)
            lse_a = mine_lse[i, s, :, 0:1]
            m = jnp.maximum(lse_a, lse_b)
            w_a, w_b = jnp.exp2(lse_a - m), jnp.exp2(lse_b - m)
            inv = 1.0 / (w_a + w_b)
            o = mine[i, s] * (w_a * inv) + ici_recv[i, s].astype(F32) * (w_b * inv)
            out_buf[PAIR * i + s] = o.astype(BF16).reshape(toks, heads, LATENT)

    def step(i, compute, merging, sending, first=False):
        if sending:
            out_send(i - 3).start()

            def send_lse():
                lse_send_copy((i - 2) // LSE_STEPS - 1).start()

            if isinstance(i, int):
                if i > steps:
                    lse_send_copy(steps // LSE_STEPS + i - steps - 2).start()
            else:
                pl.when(lax.rem(i - 2, LSE_STEPS) == 0)(send_lse)
        if merging:
            part_copy(i - 2).wait()
        if compute or merging:
            if not first:
                if isinstance(i, int) and i - 1 >= steps:
                    pass
                else:
                    part_copy(i - 1).start()
        if compute:
            for s in range(PAIR):
                kv_copy(i, s).wait()

            def prefetch():
                for s in range(PAIR):
                    kv_copy(i + DEPTH - 1, s).start()

            def forward():
                q_send(i + 1, 1).wait_recv()
                q_send(i + 1, 2).start()

            def more():
                q_send(i + AHEAD, 1).start()
                q_send(i + AHEAD, 0).start()

            if isinstance(i, int):
                if i + DEPTH - 1 < steps:
                    prefetch()
                if i + AHEAD < steps:
                    more()
                if i + 1 < steps:
                    forward()
            else:
                pl.when(i + DEPTH - 1 < steps)(prefetch)
                pl.when(i + AHEAD < steps)(more)
                pl.when(i + 1 < steps)(forward)
            q_send(i, 0).wait_recv()
            q_send(i, 2).wait_recv()
        if merging:
            merge(i - 2)
        if compute:
            tops = [scores(i, 0, s_a), scores(i, 1, s_b)]
            attend(i, 0, s_a, p_a, tops[0])
            attend(i, 1, s_b, p_b, tops[1])

    q_send(0, 1).wait_recv()
    q_send(0, 2).start()
    step(0, True, False, False, first=True)
    step(1, True, False, False)
    step(2, True, True, False)

    def body(i, carry):
        step(i, True, True, True)
        return carry

    lax.fori_loop(3, steps, body, 0)
    step(steps, False, True, True)
    step(steps + 1, False, True, True)
    step(steps + 2, False, False, True)

    def arrive(i):
        for dest in range(3):
            q_send(i, dest).wait_send()
        out_send(i).wait()

    def tail(k, carry):
        for u in range(LSE_STEPS):
            arrive(LSE_STEPS * k + u)
        lse_send_copy(k).wait()
        for u in range(LSE_STEPS):
            finish(LSE_STEPS * k + u)
        return carry

    groups = steps // LSE_STEPS
    lax.fori_loop(0, groups - 1, tail, 0)
    for i in range(steps - LSE_STEPS, steps - 1):
        arrive(i)
    lse_send_copy(groups - 1).wait()
    for i in range(steps - LSE_STEPS, steps - 1):
        finish(i)
    arrive(steps - 1)
    lse_send_copy(groups).wait()
    finish(steps - 1)


def solution(mesh):
    def local_step(q_blk, kv_blk, len_blk):
        batch, toks, heads, width = q_blk.shape
        rounds = kv_blk.shape[1]
        seq_loc = rounds * PAGE
        steps = batch // PAIR
        rows = toks * heads
        keys = kv_blk.reshape(batch, seq_loc, width)
        wide = LATENT + LANES
        dma = pltpu.SemaphoreType.DMA
        return pl.pallas_call(
            _kernel,
            out_shape=pltpu.VMEM((batch, toks, heads, LATENT), BF16),
            in_specs=[
                pl.BlockSpec(memory_space=pltpu.SMEM),
                pl.BlockSpec(memory_space=pl.ANY),
                pl.BlockSpec(memory_space=pl.ANY),
            ],
            out_specs=pl.BlockSpec(memory_space=pltpu.VMEM),
            scratch_shapes=[
                pltpu.VMEM((batch, toks, heads, width), BF16),
                pltpu.VMEM((4, batch, toks * width // LANES, heads, LANES), BF16),
                pltpu.VMEM((DEPTH, PAIR, seq_loc, width), BF16),
                pltpu.VMEM((4 * rows, seq_loc), F32),
                pltpu.VMEM((4 * rows, seq_loc), F32),
                pltpu.VMEM((4 * rows, seq_loc), BF16),
                pltpu.VMEM((4 * rows, seq_loc), BF16),
                pltpu.VMEM((2, PAIR, 2 * rows, wide), F32),
                pltpu.VMEM((2, PAIR, 2 * rows, wide), F32),
                pltpu.VMEM((steps, PAIR, 2 * rows, wide), F32),
                pltpu.VMEM((steps, PAIR, rows, LATENT), F32),
                pltpu.VMEM((steps, PAIR, rows, LANES), F32),
                pltpu.VMEM((steps, PAIR, rows, LATENT), BF16),
                pltpu.VMEM((steps, PAIR, rows, LATENT), BF16),
                pltpu.VMEM((steps // LSE_STEPS + 1, LSE_STEPS, LANES), F32),
                pltpu.VMEM((steps // LSE_STEPS + 1, LSE_STEPS, LANES), F32),
                dma((3,)),
                dma((DEPTH, PAIR)),
                dma((3, steps)),
                dma((3, steps)),
                dma((2,)),
                dma((steps,)),
                dma((2, steps)),
                dma((2, steps)),
            ],
            compiler_params=pltpu.CompilerParams(
                collective_id=0, has_side_effects=True, vmem_limit_bytes=60_000_000),
            name='mla_decode',
        )(len_blk, q_blk, keys)

    return jax.shard_map(
        local_step, mesh=mesh,
        in_specs=(P('dp', None, 'dcp', None), P('dp', None, 'dcp', None, None), P('dp')),
        out_specs=P('dp', None, 'dcp', None), check_vma=False)
```

```python
import functools
import math

import jax
import jax.numpy as jnp
from jax import lax
from jax.experimental import pallas as pl
from jax.experimental.pallas import tpu as pltpu
from jax.sharding import PartitionSpec as P

LATENT = 512
ROPE = 64
NOPE = 128
PAGE = 64
MASKED = -1e30
LANES = 128
PAIR = 2
FIRST = 2
AHEAD = 8
LSE_STEPS = 4
DEPTH = 3
MESH_ID = pl.DeviceIdType.MESH
F32 = jnp.float32
BF16 = jnp.bfloat16


def _nt_dot(a, b):
    return lax.dot_general(a, b, (((1,), (1,)), ((), ())), preferred_element_type=F32)


def _mod(i, n):
    return i % n if isinstance(i, int) else lax.rem(i, n)


def _kernel(len_hbm, q_hbm, kv_hbm, out_buf,
            len_ref, q_own, q_msg, kv_buf, s_a, s_b, p_a, p_b,
            keep, part_send, part_recv, mine, mine_lse,
            ici_send, ici_recv, lse_send, lse_recv,
            own_sem, kv_sem, qs_sem, qr_sem, part_ssem, part_rsem, ici_ssem, ici_rsem):
    batch, toks, heads, width = q_own.shape
    steps = batch // PAIR
    seq_loc = kv_buf.shape[2]
    rows = toks * heads
    tile = LANES
    group = 4
    me = lax.axis_index('dcp')
    core = lax.rem(me, 2)
    partner = me + 1 - 2 * core
    across = lax.rem(me + 2, group)

    barrier = pltpu.get_barrier_semaphore()
    for peer in (partner, across):
        pl.semaphore_signal(barrier, inc=1, device_id={'dcp': peer}, device_id_type=MESH_ID)

    cuts = (0, PAIR * FIRST, PAIR * AHEAD, batch)
    own_copies = []
    for k in range(3):
        at = pl.ds(cuts[k], cuts[k + 1] - cuts[k])
        own_copies.append(pltpu.make_async_copy(q_hbm.at[at], q_own.at[at], own_sem.at[k]))
        own_copies[-1].start()

    len_copy = pltpu.make_async_copy(len_hbm, len_ref, own_sem.at[3])
    len_copy.start()

    def kv_copy(i, s):
        slot = _mod(i, DEPTH)
        return pltpu.make_async_copy(kv_hbm.at[PAIR * i + s], kv_buf.at[slot, s], kv_sem.at[slot, s])

    def pair(i):
        return pl.ds(PAIR * i, PAIR)

    q_msgs = steps // 2 + 1

    def q_send(m, dest):
        slot = (2, 1, 3)[dest]
        if isinstance(m, int) and m < 2:
            at = pl.ds(PAIR * m, PAIR)
        else:
            at = pl.ds(2 * PAIR * (m - 1), 2 * PAIR)
        return pltpu.make_async_remote_copy(
            src_ref=q_msg.at[1 if dest == 2 else 0, at], dst_ref=q_msg.at[slot, at],
            send_sem=qs_sem.at[dest, m], recv_sem=qr_sem.at[slot - 1, m],
            device_id={'dcp': (partner, across, partner)[dest]}, device_id_type=MESH_ID)

    def part_copy(i):
        slot = _mod(i, 2)
        return pltpu.make_async_remote_copy(
            src_ref=part_send.at[slot], dst_ref=part_recv.at[i],
            send_sem=part_ssem.at[slot], recv_sem=part_rsem.at[i],
            device_id={'dcp': partner}, device_id_type=MESH_ID)

    out_msgs = steps // 2 + 1

    def out_send(m):
        if isinstance(m, int) and m >= out_msgs - 2:
            at = pl.ds(m + steps - out_msgs, 1)
        else:
            at = pl.ds(2 * m, 2)
        return pltpu.make_async_remote_copy(
            src_ref=ici_send.at[at], dst_ref=ici_recv.at[at],
            send_sem=ici_ssem.at[0, m], recv_sem=ici_rsem.at[0, m],
            device_id={'dcp': across}, device_id_type=MESH_ID)

    groups = steps // LSE_STEPS

    def lse_row(i):
        if isinstance(i, int) and i == steps - 1:
            return groups, 0
        return i // LSE_STEPS, _mod(i, LSE_STEPS) // 2

    def lse_send_copy(k):
        return pltpu.make_async_remote_copy(
            src_ref=lse_send.at[k], dst_ref=lse_recv.at[k],
            send_sem=ici_ssem.at[1, k], recv_sem=ici_rsem.at[1, k],
            device_id={'dcp': across}, device_id_type=MESH_ID)

    unroll = PAIR * FIRST
    lat_tiles = LATENT // LANES

    def pack(k, carry):
        for u in range(unroll):
            b = unroll * k + u
            for t in range(toks):
                for n in range(lat_tiles):
                    q_msg[0, b, t * lat_tiles + n] = q_own[b, t, :, n * LANES:(n + 1) * LANES]
            q_msg[0, b, toks * lat_tiles] = jnp.concatenate(
                [q_own[b, t, :, LATENT:width] for t in range(toks)], axis=-1)
        return carry

    own_copies[0].wait()
    pack(0, 0)
    pl.semaphore_wait(barrier, 2)
    for k in range(2):
        if k == 1:
            own_copies[1].wait()
            lax.fori_loop(1, cuts[2] // unroll, pack, 0)
        for m in ((0, 1), range(2, AHEAD // 2 + 1))[k]:
            q_send(m, 1).start()
            q_send(m, 0).start()
    for i in range(DEPTH - 1):
        for s in range(PAIR):
            kv_copy(i, s).start()
    len_copy.wait()
    own_copies[2].wait()
    lax.fori_loop(cuts[2] // unroll, batch // unroll, pack, 0)

    scale2 = (NOPE + ROPE) ** -0.5 * math.log2(math.e)
    row_tok = lax.rem(lax.broadcasted_iota(jnp.int32, (group * rows, 1), 0) // heads, toks)
    col = lax.broadcasted_iota(jnp.int32, (1, seq_loc), 1)
    col_pos = (col // PAGE) * (group * PAGE) + lax.rem(col, PAGE) + me * PAGE
    half = lax.broadcasted_iota(jnp.int32, (group * rows // 2, LANES), 1) < LANES // 2

    def load_q(b):
        lat = jnp.concatenate(
            [jnp.concatenate([q_msg[g, b, t * lat_tiles + n] for n in range(lat_tiles)], axis=1)
             for g in range(group) for t in range(toks)], axis=0)
        rope = jnp.concatenate(
            [q_msg[g, b, toks * lat_tiles][:, t * ROPE:(t + 1) * ROPE]
             for g in range(group) for t in range(toks)], axis=0)
        return lat, rope

    def scores(i, s, s_ref):
        slot = _mod(i, DEPTH)
        b = PAIR * i + s
        lat, rope = load_q(b)
        last = len_ref[b] - toks + row_tok
        best = None
        chunk = 512
        for n in range(seq_loc // chunk):
            at = pl.ds(n * chunk, chunk)
            sc = _nt_dot(lat, kv_buf[slot, s, at, 0:LATENT]) + _nt_dot(rope, kv_buf[slot, s, at, LATENT:width])
            sc = jnp.where(col_pos[:, n * chunk:(n + 1) * chunk] <= last, sc * scale2, MASKED)
            s_ref[:, at] = sc
            for t in range(chunk // tile):
                piece = sc[:, t * tile:(t + 1) * tile]
                best = piece if best is None else jnp.maximum(best, piece)
        return jnp.max(best, axis=1, keepdims=True)

    def attend(i, s, s_ref, p_ref, top):
        slot, held = _mod(i, 2), _mod(i, DEPTH)
        total = None
        for n in range(seq_loc // tile):
            w = jnp.exp2(s_ref[:, n * tile:(n + 1) * tile] - top)
            total = w if total is None else total + w
            p_ref[:, n * tile:(n + 1) * tile] = w.astype(BF16)
        out = jnp.dot(p_ref[...], kv_buf[held, s, :, 0:LATENT], preferred_element_type=F32)
        norm = jnp.sum(total, axis=1, keepdims=True)
        stats = jnp.where(half[0:1], top, norm)
        h = group * rows // 2
        keep[slot, s, :, 0:LATENT] = out[:h]
        keep[slot, s, :, LATENT:LATENT + LANES] = stats[:h]
        part_send[slot, s, :, 0:LATENT] = out[h:]
        part_send[slot, s, :, LATENT:LATENT + LANES] = stats[h:]

    row_id = lax.broadcasted_iota(jnp.int32, (rows, LANES), 0)
    lane_id = lax.broadcasted_iota(jnp.int32, (rows, LANES), 1)

    def merge(i):
        slot = _mod(i, 2)
        lse_sum = None
        for s in range(PAIR):
            st_a = keep[slot, s, :, LATENT:LATENT + LANES]
            st_b = part_recv[i, s, :, LATENT:LATENT + LANES]
            m_a, l_a = st_a[:, 0:1], st_a[:, LANES // 2:LANES // 2 + 1]
            m_b, l_b = st_b[:, 0:1], st_b[:, LANES // 2:LANES // 2 + 1]
            m = jnp.maximum(m_a, m_b)
            w_a, w_b = jnp.exp2(m_a - m), jnp.exp2(m_b - m)
            norm = l_a * w_a + l_b * w_b
            lse = m + jnp.log2(norm)
            inv = 1.0 / norm
            both = keep[slot, s, :, 0:LATENT] * (w_a * inv) + part_recv[i, s, :, 0:LATENT] * (w_b * inv)
            mine[i, s] = both[:rows]
            ici_send[i, s] = both[rows:].astype(BF16)
            wide = jnp.broadcast_to(lse, (2 * rows, LANES))
            mine_lse[i, s] = wide[:rows]
            picked = jnp.where(lane_id == row_id + (s * rows + PAIR * rows * _mod(i, 2)), wide[rows:], 0.0)
            lse_sum = picked if lse_sum is None else lse_sum + picked
        k, r = lse_row(i)
        line = jnp.sum(lse_sum, axis=0, keepdims=True)
        before = lse_send[k, pl.ds(r, 1)]
        lse_send[k, pl.ds(r, 1)] = jnp.where(lane_id[0:1] // (PAIR * rows) == _mod(i, 2), line, before)

    def finish(i):
        k, r = lse_row(i)
        row = jnp.broadcast_to(lse_recv[k, pl.ds(r, 1)], (rows, LANES))
        for s in range(PAIR):
            lane = row_id + (s * rows + PAIR * rows * _mod(i, 2))
            lse_b = jnp.sum(jnp.where(lane_id == lane, row, 0.0), axis=1, keepdims=True)
            lse_a = mine_lse[i, s, :, 0:1]
            m = jnp.maximum(lse_a, lse_b)
            w_a, w_b = jnp.exp2(lse_a - m), jnp.exp2(lse_b - m)
            inv = 1.0 / (w_a + w_b)
            o = mine[i, s] * (w_a * inv) + ici_recv[i, s].astype(F32) * (w_b * inv)
            out_buf[PAIR * i + s] = o.astype(BF16).reshape(toks, heads, LATENT)

    def when(i, parity, limit, action):
        if isinstance(i, int):
            if i % 2 == parity and i < limit:
                action()
        else:
            pl.when(jnp.logical_and(lax.rem(i, 2) == parity, i < limit))(action)

    def step(i, compute=True, merging=True):
        if merging:
            part_copy(i - 2).wait()
        if not (isinstance(i, int) and i == 0):
            part_copy(i - 1).start()
        if compute:
            for s in range(PAIR):
                kv_copy(i, s).wait()

            def prefetch():
                for s in range(PAIR):
                    kv_copy(i + DEPTH - 1, s).start()

            def more():
                m = (i + AHEAD) // 2 + 1
                q_send(m, 1).start()
                q_send(m, 0).start()

            def forward():
                m = (i + 1) // 2 + 1
                q_send(m, 1).wait_recv()
                q_send(m, 2).start()

            def arrived():
                q_send(i // 2 + 1, 0).wait_recv()
                q_send(i // 2 + 1, 2).wait_recv()

            if isinstance(i, int):
                if i + DEPTH - 1 < steps:
                    prefetch()
            else:
                pl.when(i + DEPTH - 1 < steps)(prefetch)
            when(i, 0, steps - AHEAD, more)
            if isinstance(i, int) and i == 0:
                q_send(1, 1).wait_recv()
                q_send(1, 2).start()
            else:
                when(i, 1, steps - 1, forward)
            if isinstance(i, int) and i < 2:
                for dest in (0, 2):
                    q_send(i, dest).wait_recv()
            else:
                when(i, 0, steps, arrived)
        if merging:
            merge(i - 2)
        if compute:
            tops = [scores(i, 0, s_a), scores(i, 1, s_b)]
            attend(i, 0, s_a, p_a, tops[0])
            attend(i, 1, s_b, p_b, tops[1])

    def send_out(i):
        out_send(i // 2 - 2).start()

        def send_lse():
            lse_send_copy((i - 2) // LSE_STEPS - 1).start()

        if isinstance(i, int):
            if (i - 2) % LSE_STEPS == 0:
                send_lse()
        else:
            pl.when(lax.rem(i - 2, LSE_STEPS) == 0)(send_lse)

    q_send(0, 1).wait_recv()
    q_send(0, 2).start()
    step(0, merging=False)
    step(1, merging=False)
    step(2)

    def body(i, carry):
        when(i, 0, steps, lambda: send_out(i))
        step(i)
        return carry

    lax.fori_loop(3, steps, body, 0)
    send_out(steps)
    step(steps, compute=False)
    part_copy(steps - 1).wait()
    merge(steps - 1)
    lse_send_copy(groups - 1).start()
    out_send(out_msgs - 2).start()
    lse_send_copy(groups).start()
    out_send(out_msgs - 1).start()

    for dest in range(3):
        for m in range(2):
            q_send(m, dest).wait_send()

    def q_sent(m, carry):
        for dest in range(3):
            q_send(m, dest).wait_send()
        return carry

    lax.fori_loop(2, q_msgs, q_sent, 0)

    def tail(k, carry):
        for u in range(LSE_STEPS // 2):
            out_send(LSE_STEPS // 2 * k + u).wait()
        lse_send_copy(k).wait()
        for u in range(LSE_STEPS):
            finish(LSE_STEPS * k + u)
        return carry

    lax.fori_loop(0, groups - 1, tail, 0)
    out_send(out_msgs - 3).wait()
    lse_send_copy(groups - 1).wait()
    for i in range(steps - LSE_STEPS, steps - 2):
        finish(i)
    out_send(out_msgs - 2).wait()
    finish(steps - 2)
    lse_send_copy(groups).wait()
    out_send(out_msgs - 1).wait()
    finish(steps - 1)


def solution(mesh):
    def local_step(q_blk, kv_blk, len_blk):
        batch, toks, heads, width = q_blk.shape
        rounds = kv_blk.shape[1]
        seq_loc = rounds * PAGE
        steps = batch // PAIR
        rows = toks * heads
        keys = kv_blk.reshape(batch, seq_loc, width)
        wide = LATENT + LANES
        dma = pltpu.SemaphoreType.DMA
        return pl.pallas_call(
            _kernel,
            out_shape=pltpu.VMEM((batch, toks, heads, LATENT), BF16),
            in_specs=[
                pl.BlockSpec(memory_space=pl.ANY),
                pl.BlockSpec(memory_space=pl.ANY),
                pl.BlockSpec(memory_space=pl.ANY),
            ],
            out_specs=pl.BlockSpec(memory_space=pltpu.VMEM),
            scratch_shapes=[
                pltpu.SMEM((batch,), jnp.int32),
                pltpu.VMEM((batch, toks, heads, width), BF16),
                pltpu.VMEM((4, batch, toks * width // LANES, heads, LANES), BF16),
                pltpu.VMEM((DEPTH, PAIR, seq_loc, width), BF16),
                pltpu.VMEM((4 * rows, seq_loc), F32),
                pltpu.VMEM((4 * rows, seq_loc), F32),
                pltpu.VMEM((4 * rows, seq_loc), BF16),
                pltpu.VMEM((4 * rows, seq_loc), BF16),
                pltpu.VMEM((2, PAIR, 2 * rows, wide), F32),
                pltpu.VMEM((2, PAIR, 2 * rows, wide), F32),
                pltpu.VMEM((steps, PAIR, 2 * rows, wide), F32),
                pltpu.VMEM((steps, PAIR, rows, LATENT), F32),
                pltpu.VMEM((steps, PAIR, rows, LANES), F32),
                pltpu.VMEM((steps, PAIR, rows, LATENT), BF16),
                pltpu.VMEM((steps, PAIR, rows, LATENT), BF16),
                pltpu.VMEM((steps // LSE_STEPS + 1, LSE_STEPS // 2, LANES), F32),
                pltpu.VMEM((steps // LSE_STEPS + 1, LSE_STEPS // 2, LANES), F32),
                dma((4,)),
                dma((DEPTH, PAIR)),
                dma((3, steps // 2 + 1)),
                dma((3, steps // 2 + 1)),
                dma((2,)),
                dma((steps,)),
                dma((2, steps // 2 + 1)),
                dma((2, steps // 2 + 1)),
            ],
            compiler_params=pltpu.CompilerParams(
                collective_id=0, has_side_effects=True, vmem_limit_bytes=60_000_000),
            name='mla_decode',
        )(len_blk, q_blk, keys)

    return jax.shard_map(
        local_step, mesh=mesh,
        in_specs=(P('dp', None, 'dcp', None), P('dp', None, 'dcp', None, None), P('dp')),
        out_specs=P('dp', None, 'dcp', None), check_vma=False)
```

```python
import functools
import math

import jax
import jax.numpy as jnp
from jax import lax
from jax.experimental import pallas as pl
from jax.experimental.pallas import tpu as pltpu
from jax.sharding import PartitionSpec as P

LATENT = 512
ROPE = 64
NOPE = 128
PAGE = 64
MASKED = -1e30
LANES = 128
PAIR = 2
FIRST = 2
AHEAD = 12
MSG = 4
DEPTH = 3
MESH_ID = pl.DeviceIdType.MESH
F32 = jnp.float32
BF16 = jnp.bfloat16


def _nt_dot(a, b):
    return lax.dot_general(a, b, (((1,), (1,)), ((), ())), preferred_element_type=F32)


def _mod(i, n):
    return i % n if isinstance(i, int) else lax.rem(i, n)


def _kernel(len_hbm, q_hbm, kv_hbm, out_buf,
            len_ref, q_own, q_msg, kv_buf, s_a, s_b, p_a, p_b,
            keep, part_send, part_recv, mine, mine_lse,
            ici_send, ici_recv, lse_send, lse_recv,
            own_sem, kv_sem, qs_sem, qr_sem, part_ssem, part_rsem, ici_ssem, ici_rsem):
    batch, toks, heads, width = q_own.shape
    steps = batch // PAIR
    seq_loc = kv_buf.shape[2]
    rows = toks * heads
    tile = LANES
    group = 4
    me = lax.axis_index('dcp')
    core = lax.rem(me, 2)
    partner = me + 1 - 2 * core
    across = lax.rem(me + 2, group)

    barrier = pltpu.get_barrier_semaphore()
    for peer in (partner, across):
        pl.semaphore_signal(barrier, inc=1, device_id={'dcp': peer}, device_id_type=MESH_ID)

    cuts = (0, PAIR * FIRST, PAIR * AHEAD, batch)
    own_copies = []
    for k in range(3):
        at = pl.ds(cuts[k], cuts[k + 1] - cuts[k])
        own_copies.append(pltpu.make_async_copy(q_hbm.at[at], q_own.at[at], own_sem.at[k]))
        own_copies[-1].start()

    len_copy = pltpu.make_async_copy(len_hbm, len_ref, own_sem.at[3])
    len_copy.start()

    def kv_copy(i, s):
        slot = _mod(i, DEPTH)
        return pltpu.make_async_copy(kv_hbm.at[PAIR * i + s], kv_buf.at[slot, s], kv_sem.at[slot, s])

    def pair(i):
        return pl.ds(PAIR * i, PAIR)

    heads_of = ((0, 1), (1, 1), (2, 2), (4, 2), (6, 2))
    q_msgs = steps // MSG + 3

    def q_send(m, dest):
        slot = (2, 1, 3)[dest]
        first, count = heads_of[m] if isinstance(m, int) and m < 5 else (MSG * (m - 3), MSG)
        at = pl.ds(PAIR * first, PAIR * count)
        return pltpu.make_async_remote_copy(
            src_ref=q_msg.at[1 if dest == 2 else 0, at], dst_ref=q_msg.at[slot, at],
            send_sem=qs_sem.at[dest, m], recv_sem=qr_sem.at[slot - 1, m],
            device_id={'dcp': (partner, across, partner)[dest]}, device_id_type=MESH_ID)

    def part_copy(i):
        slot = _mod(i, 2)
        return pltpu.make_async_remote_copy(
            src_ref=part_send.at[slot], dst_ref=part_recv.at[i],
            send_sem=part_ssem.at[slot], recv_sem=part_rsem.at[i],
            device_id={'dcp': partner}, device_id_type=MESH_ID)

    groups = steps // MSG
    long = groups - 2
    last_of = ((steps - 8, 2), (steps - 6, 2), (steps - 4, 2), (steps - 2, 1), (steps - 1, 1))

    def out_send(m):
        first, count = last_of[m - long] if isinstance(m, int) and m >= long else (MSG * m, MSG)
        at = pl.ds(first, count)
        return pltpu.make_async_remote_copy(
            src_ref=ici_send.at[at], dst_ref=ici_recv.at[at],
            send_sem=ici_ssem.at[0, m], recv_sem=ici_rsem.at[0, m],
            device_id={'dcp': across}, device_id_type=MESH_ID)

    def lse_row(i):
        if isinstance(i, int) and i == steps - 1:
            return groups, 0
        return i // MSG, _mod(i, MSG) // 2

    def lse_send_copy(k):
        return pltpu.make_async_remote_copy(
            src_ref=lse_send.at[k], dst_ref=lse_recv.at[k],
            send_sem=ici_ssem.at[1, k], recv_sem=ici_rsem.at[1, k],
            device_id={'dcp': across}, device_id_type=MESH_ID)

    unroll = PAIR * FIRST
    lat_tiles = LATENT // LANES

    def pack(k, carry):
        for u in range(unroll):
            b = unroll * k + u
            for t in range(toks):
                for n in range(lat_tiles):
                    q_msg[0, b, t * lat_tiles + n] = q_own[b, t, :, n * LANES:(n + 1) * LANES]
            q_msg[0, b, toks * lat_tiles] = jnp.concatenate(
                [q_own[b, t, :, LATENT:width] for t in range(toks)], axis=-1)
        return carry

    own_copies[0].wait()
    pack(0, 0)
    pl.semaphore_wait(barrier, 2)
    for k in range(2):
        if k == 1:
            own_copies[1].wait()
            lax.fori_loop(1, cuts[2] // unroll, pack, 0)
        for m in ((0, 1), range(2, AHEAD // MSG + 3))[k]:
            q_send(m, 1).start()
            q_send(m, 0).start()
    for i in range(DEPTH - 1):
        for s in range(PAIR):
            kv_copy(i, s).start()
    len_copy.wait()
    own_copies[2].wait()
    lax.fori_loop(cuts[2] // unroll, batch // unroll, pack, 0)

    scale2 = (NOPE + ROPE) ** -0.5 * math.log2(math.e)
    row_tok = lax.rem(lax.broadcasted_iota(jnp.int32, (group * rows, 1), 0) // heads, toks)
    col = lax.broadcasted_iota(jnp.int32, (1, seq_loc), 1)
    col_pos = (col // PAGE) * (group * PAGE) + lax.rem(col, PAGE) + me * PAGE
    always = seq_loc // 2 - PAGE
    half = lax.broadcasted_iota(jnp.int32, (group * rows // 2, LANES), 1) < LANES // 2

    def load_q(b):
        lat = jnp.concatenate(
            [jnp.concatenate([q_msg[g, b, t * lat_tiles + n] for n in range(lat_tiles)], axis=1)
             for g in range(group) for t in range(toks)], axis=0)
        rope = jnp.concatenate(
            [q_msg[g, b, toks * lat_tiles][:, t * ROPE:(t + 1) * ROPE]
             for g in range(group) for t in range(toks)], axis=0)
        return jnp.concatenate([lat, rope], axis=1)

    def scores(i, s, s_ref):
        slot = _mod(i, DEPTH)
        b = PAIR * i + s
        query = load_q(b)
        last = len_ref[b] - toks + row_tok
        best = None
        chunk = 512
        for n in range(seq_loc // chunk):
            at = pl.ds(n * chunk, chunk)
            sc = _nt_dot(query, kv_buf[slot, s, at, :])
            for t in range(chunk // tile):
                lo = n * chunk + t * tile
                piece = sc[:, t * tile:(t + 1) * tile] * scale2
                if lo + tile > always:
                    piece = jnp.where(col_pos[:, lo:lo + tile] <= last, piece, MASKED)
                s_ref[:, lo:lo + tile] = piece
                best = piece if best is None else jnp.maximum(best, piece)
        return jnp.max(best, axis=1, keepdims=True)

    def attend(i, s, s_ref, p_ref, top):
        slot, held = _mod(i, 2), _mod(i, DEPTH)
        total = None
        for n in range(seq_loc // tile):
            w = jnp.exp2(s_ref[:, n * tile:(n + 1) * tile] - top)
            total = w if total is None else total + w
            p_ref[:, n * tile:(n + 1) * tile] = w.astype(BF16)
        out = jnp.dot(p_ref[...], kv_buf[held, s, :, 0:LATENT], preferred_element_type=F32)
        norm = jnp.sum(total, axis=1, keepdims=True)
        stats = jnp.where(half[0:1], top, norm)
        h = group * rows // 2
        keep[slot, s, :, 0:LATENT] = out[:h]
        keep[slot, s, :, LATENT:LATENT + LANES] = stats[:h]
        part_send[slot, s, :, 0:LATENT] = out[h:]
        part_send[slot, s, :, LATENT:LATENT + LANES] = stats[h:]

    row_id = lax.broadcasted_iota(jnp.int32, (rows, LANES), 0)
    lane_id = lax.broadcasted_iota(jnp.int32, (rows, LANES), 1)

    def merge(i):
        slot = _mod(i, 2)
        lse_sum = None
        for s in range(PAIR):
            st_a = keep[slot, s, :, LATENT:LATENT + LANES]
            st_b = part_recv[i, s, :, LATENT:LATENT + LANES]
            m_a, l_a = st_a[:, 0:1], st_a[:, LANES // 2:LANES // 2 + 1]
            m_b, l_b = st_b[:, 0:1], st_b[:, LANES // 2:LANES // 2 + 1]
            m = jnp.maximum(m_a, m_b)
            w_a, w_b = jnp.exp2(m_a - m), jnp.exp2(m_b - m)
            norm = l_a * w_a + l_b * w_b
            lse = m + jnp.log2(norm)
            inv = 1.0 / norm
            both = keep[slot, s, :, 0:LATENT] * (w_a * inv) + part_recv[i, s, :, 0:LATENT] * (w_b * inv)
            mine[i, s] = both[:rows]
            ici_send[i, s] = both[rows:].astype(BF16)
            wide = jnp.broadcast_to(lse, (2 * rows, LANES))
            mine_lse[i, s] = wide[:rows]
            picked = jnp.where(lane_id == row_id + (s * rows + PAIR * rows * _mod(i, 2)), wide[rows:], 0.0)
            lse_sum = picked if lse_sum is None else lse_sum + picked
        k, r = lse_row(i)
        line = jnp.sum(lse_sum, axis=0, keepdims=True)
        before = lse_send[k, pl.ds(r, 1)]
        lse_send[k, pl.ds(r, 1)] = jnp.where(lane_id[0:1] // (PAIR * rows) == _mod(i, 2), line, before)

    def finish_weights(i):
        k, r = lse_row(i)
        row = jnp.broadcast_to(lse_recv[k, pl.ds(r, 1)], (rows, LANES))
        weights = []
        for s in range(PAIR):
            lane = row_id + (s * rows + PAIR * rows * _mod(i, 2))
            lse_b = jnp.sum(jnp.where(lane_id == lane, row, 0.0), axis=1, keepdims=True)
            lse_a = mine_lse[i, s, :, 0:1]
            m = jnp.maximum(lse_a, lse_b)
            w_a, w_b = jnp.exp2(lse_a - m), jnp.exp2(lse_b - m)
            inv = 1.0 / (w_a + w_b)
            weights.append((w_a * inv, w_b * inv))
        return weights

    def finish(i, weights=None):
        weights = finish_weights(i) if weights is None else weights
        for s in range(PAIR):
            o = mine[i, s] * weights[s][0] + ici_recv[i, s].astype(F32) * weights[s][1]
            out_buf[PAIR * i + s] = o.astype(BF16).reshape(toks, heads, LATENT)

    def when(i, phase, limit, action):
        if isinstance(i, int):
            if i % MSG == phase and i < limit:
                action()
        else:
            pl.when(jnp.logical_and(lax.rem(i, MSG) == phase, i < limit))(action)

    def step(i, compute=True, merging=True):
        if merging:
            part_copy(i - 2).wait()
        if not (isinstance(i, int) and i == 0):
            part_copy(i - 1).start()
        if compute:
            for s in range(PAIR):
                kv_copy(i, s).wait()

            def prefetch():
                for s in range(PAIR):
                    kv_copy(i + DEPTH - 1, s).start()

            def more():
                m = (i + AHEAD) // MSG + 3
                q_send(m, 1).start()
                q_send(m, 0).start()

            def forward(m):
                q_send(m, 1).wait_recv()
                q_send(m, 2).start()

            def arrived(m):
                q_send(m, 0).wait_recv()
                q_send(m, 2).wait_recv()

            if isinstance(i, int):
                if i + DEPTH - 1 < steps:
                    prefetch()
            else:
                pl.when(i + DEPTH - 1 < steps)(prefetch)
            when(i, 0, steps - AHEAD, more)
            if isinstance(i, int):
                if i < 2:
                    forward(i + 1)
                arrived(i)
            else:
                for m in (3, 4):
                    pl.when(i == heads_of[m][0] - 1)(functools.partial(forward, m))
                    pl.when(i == heads_of[m][0])(functools.partial(arrived, m))
                late = i > heads_of[4][0]
                pl.when(jnp.logical_and(late, jnp.logical_and(lax.rem(i, MSG) == MSG - 1, i < steps - 1)))(
                    lambda: forward((i + 1) // MSG + 3))
                pl.when(jnp.logical_and(late, lax.rem(i, MSG) == 0))(lambda: arrived(i // MSG + 3))
        if merging:
            merge(i - 2)
        if compute:
            tops = [scores(i, 0, s_a), scores(i, 1, s_b)]
            attend(i, 0, s_a, p_a, tops[0])
            attend(i, 1, s_b, p_b, tops[1])

    def send_out(i):
        k = (i - 2) // MSG - 1
        out_send(k).start()
        lse_send_copy(k).start()

    q_send(0, 1).wait_recv()
    q_send(0, 2).start()
    step(0, merging=False)
    step(1, merging=False)
    step(2)

    def body(i, carry):
        pl.when(jnp.logical_and(lax.rem(i, MSG) == 2, jnp.logical_and(i > MSG, i < steps - 4)))(lambda: send_out(i))
        pl.when(i == steps - 4)(out_send(long).start)

        @pl.when(i == steps - 2)
        def _():
            out_send(long + 1).start()
            lse_send_copy(long).start()

        step(i)
        return carry

    lax.fori_loop(3, steps, body, 0)
    out_send(long + 2).start()
    step(steps, compute=False)
    part_copy(steps - 1).wait()
    merge(steps - 1)
    lse_send_copy(groups - 1).start()
    out_send(long + 3).start()
    lse_send_copy(groups).start()
    out_send(long + 4).start()

    def q_sent(m, carry):
        for dest in range(3):
            q_send(m, dest).wait_send()
        return carry

    for m in range(5):
        q_sent(m, 0)
    lax.fori_loop(5, q_msgs, q_sent, 0)

    def tail(k, carry):
        out_send(k).wait()
        lse_send_copy(k).wait()
        for u in range(MSG):
            finish(MSG * k + u)
        return carry

    lax.fori_loop(0, long, tail, 0)
    out_send(long).wait()
    out_send(long + 1).wait()
    lse_send_copy(long).wait()
    for i in range(steps - 8, steps - 4):
        finish(i)
    out_send(long + 2).wait()
    lse_send_copy(groups - 1).wait()
    for i in range(steps - 4, steps - 2):
        finish(i)
    weights = finish_weights(steps - 2)
    out_send(long + 3).wait()
    finish(steps - 2, weights)
    lse_send_copy(groups).wait()
    weights = finish_weights(steps - 1)
    out_send(long + 4).wait()
    finish(steps - 1, weights)


def solution(mesh):
    def local_step(q_blk, kv_blk, len_blk):
        batch, toks, heads, width = q_blk.shape
        rounds = kv_blk.shape[1]
        seq_loc = rounds * PAGE
        steps = batch // PAIR
        rows = toks * heads
        keys = kv_blk.reshape(batch, seq_loc, width)
        wide = LATENT + LANES
        dma = pltpu.SemaphoreType.DMA
        return pl.pallas_call(
            _kernel,
            out_shape=pltpu.VMEM((batch, toks, heads, LATENT), BF16),
            in_specs=[
                pl.BlockSpec(memory_space=pl.ANY),
                pl.BlockSpec(memory_space=pl.ANY),
                pl.BlockSpec(memory_space=pl.ANY),
            ],
            out_specs=pl.BlockSpec(memory_space=pltpu.VMEM),
            scratch_shapes=[
                pltpu.SMEM((batch,), jnp.int32),
                pltpu.VMEM((batch, toks, heads, width), BF16),
                pltpu.VMEM((4, batch, toks * width // LANES, heads, LANES), BF16),
                pltpu.VMEM((DEPTH, PAIR, seq_loc, width), BF16),
                pltpu.VMEM((4 * rows, seq_loc), F32),
                pltpu.VMEM((4 * rows, seq_loc), F32),
                pltpu.VMEM((4 * rows, seq_loc), BF16),
                pltpu.VMEM((4 * rows, seq_loc), BF16),
                pltpu.VMEM((2, PAIR, 2 * rows, wide), F32),
                pltpu.VMEM((2, PAIR, 2 * rows, wide), F32),
                pltpu.VMEM((steps, PAIR, 2 * rows, wide), F32),
                pltpu.VMEM((steps, PAIR, rows, LATENT), F32),
                pltpu.VMEM((steps, PAIR, rows, LANES), F32),
                pltpu.VMEM((steps, PAIR, rows, LATENT), BF16),
                pltpu.VMEM((steps, PAIR, rows, LATENT), BF16),
                pltpu.VMEM((steps // MSG + 1, MSG // 2, LANES), F32),
                pltpu.VMEM((steps // MSG + 1, MSG // 2, LANES), F32),
                dma((4,)),
                dma((DEPTH, PAIR)),
                dma((3, steps // MSG + 3)),
                dma((3, steps // MSG + 3)),
                dma((2,)),
                dma((steps,)),
                dma((2, steps // MSG + 3)),
                dma((2, steps // MSG + 3)),
            ],
            compiler_params=pltpu.CompilerParams(
                collective_id=0, has_side_effects=True, vmem_limit_bytes=60_000_000),
            name='mla_decode',
        )(len_blk, q_blk, keys)

    return jax.shard_map(
        local_step, mesh=mesh,
        in_specs=(P('dp', None, 'dcp', None), P('dp', None, 'dcp', None, None), P('dp')),
        out_specs=P('dp', None, 'dcp', None), check_vma=False)
```

```python
import functools
import math

import jax
import jax.numpy as jnp
from jax import lax
from jax.experimental import pallas as pl
from jax.experimental.pallas import tpu as pltpu
from jax.sharding import PartitionSpec as P

LATENT = 512
ROPE = 64
NOPE = 128
PAGE = 64
MASKED = -math.inf
LANES = 128
PAIR = 2
FIRST = 2
AHEAD = 12
MSG = 4
DEPTH = 3
MESH_ID = pl.DeviceIdType.MESH
F32 = jnp.float32
BF16 = jnp.bfloat16


def _nt_dot(a, b):
    return lax.dot_general(a, b, (((1,), (1,)), ((), ())), preferred_element_type=F32)


def _mod(i, n):
    return i % n if isinstance(i, int) else lax.rem(i, n)


def _kernel(len_hbm, q_hbm, kv_hbm, out_buf,
            len_ref, q_own, q_msg, kv_buf, s_a, s_b, p_a, p_b,
            keep, part_send, part_recv, mine, mine_lse,
            ici_send, ici_recv, lse_send, lse_recv,
            own_sem, kv_sem, qs_sem, qr_sem, part_ssem, part_rsem, ici_ssem, ici_rsem):
    batch, toks, heads, width = q_own.shape
    steps = batch // PAIR
    seq_loc = kv_buf.shape[2]
    rows = toks * heads
    tile = LANES
    group = 4
    me = lax.axis_index('dcp')
    core = lax.rem(me, 2)
    partner = me + 1 - 2 * core
    across = lax.rem(me + 2, group)

    barrier = pltpu.get_barrier_semaphore()
    for peer in (partner, across):
        pl.semaphore_signal(barrier, inc=1, device_id={'dcp': peer}, device_id_type=MESH_ID)

    cuts = (0, PAIR * FIRST, PAIR * AHEAD, batch)
    own_copies = []
    for k in range(3):
        at = pl.ds(cuts[k], cuts[k + 1] - cuts[k])
        own_copies.append(pltpu.make_async_copy(q_hbm.at[at], q_own.at[at], own_sem.at[k]))
        own_copies[-1].start()

    len_copy = pltpu.make_async_copy(len_hbm, len_ref, own_sem.at[3])
    len_copy.start()

    def kv_copy(i, s):
        slot = _mod(i, DEPTH)
        return pltpu.make_async_copy(kv_hbm.at[PAIR * i + s], kv_buf.at[slot, s], kv_sem.at[slot, s])

    def pair(i):
        return pl.ds(PAIR * i, PAIR)

    heads_of = ((0, 1), (1, 1), (2, 2), (4, 2), (6, 2))
    q_msgs = steps // MSG + 3

    def q_send(m, dest):
        slot = (2, 1, 3)[dest]
        first, count = heads_of[m] if isinstance(m, int) and m < 5 else (MSG * (m - 3), MSG)
        at = pl.ds(PAIR * first, PAIR * count)
        return pltpu.make_async_remote_copy(
            src_ref=q_msg.at[1 if dest == 2 else 0, at], dst_ref=q_msg.at[slot, at],
            send_sem=qs_sem.at[dest, m], recv_sem=qr_sem.at[slot - 1, m],
            device_id={'dcp': (partner, across, partner)[dest]}, device_id_type=MESH_ID)

    def part_copy(i):
        slot = _mod(i, 2)
        return pltpu.make_async_remote_copy(
            src_ref=part_send.at[slot], dst_ref=part_recv.at[i],
            send_sem=part_ssem.at[slot], recv_sem=part_rsem.at[i],
            device_id={'dcp': partner}, device_id_type=MESH_ID)

    groups = steps // MSG
    long = groups - 2
    last_of = ((steps - 8, 2), (steps - 6, 2), (steps - 4, 2), (steps - 2, 1), (steps - 1, 1))

    def out_send(m):
        first, count = last_of[m - long] if isinstance(m, int) and m >= long else (MSG * m, MSG)
        at = pl.ds(first, count)
        return pltpu.make_async_remote_copy(
            src_ref=ici_send.at[at], dst_ref=ici_recv.at[at],
            send_sem=ici_ssem.at[0, m], recv_sem=ici_rsem.at[0, m],
            device_id={'dcp': across}, device_id_type=MESH_ID)

    def lse_row(i):
        if isinstance(i, int) and i == steps - 1:
            return groups, 0
        return i // MSG, _mod(i, MSG) // 2

    def lse_send_copy(k):
        return pltpu.make_async_remote_copy(
            src_ref=lse_send.at[k], dst_ref=lse_recv.at[k],
            send_sem=ici_ssem.at[1, k], recv_sem=ici_rsem.at[1, k],
            device_id={'dcp': across}, device_id_type=MESH_ID)

    unroll = PAIR * FIRST
    lat_tiles = LATENT // LANES

    def pack(k, carry):
        for u in range(unroll):
            b = unroll * k + u
            for t in range(toks):
                for n in range(lat_tiles):
                    q_msg[0, b, t * lat_tiles + n] = q_own[b, t, :, n * LANES:(n + 1) * LANES]
            q_msg[0, b, toks * lat_tiles] = jnp.concatenate(
                [q_own[b, t, :, LATENT:width] for t in range(toks)], axis=-1)
        return carry

    own_copies[0].wait()
    pack(0, 0)
    pl.semaphore_wait(barrier, 2)
    for k in range(2):
        if k == 1:
            own_copies[1].wait()
            lax.fori_loop(1, cuts[2] // unroll, pack, 0)
        for m in ((0, 1), range(2, AHEAD // MSG + 3))[k]:
            q_send(m, 1).start()
            q_send(m, 0).start()
    for i in range(DEPTH - 1):
        for s in range(PAIR):
            kv_copy(i, s).start()
    len_copy.wait()
    own_copies[2].wait()
    lax.fori_loop(cuts[2] // unroll, batch // unroll, pack, 0)

    scale2 = (NOPE + ROPE) ** -0.5 * math.log2(math.e)
    row_tok = lax.rem(lax.broadcasted_iota(jnp.int32, (group * rows, 1), 0) // heads, toks)
    col = lax.broadcasted_iota(jnp.int32, (1, seq_loc), 1)
    col_pos = (col // PAGE) * (group * PAGE) + lax.rem(col, PAGE) + me * PAGE
    always = seq_loc // 2 - PAGE
    half = lax.broadcasted_iota(jnp.int32, (group * rows // 2, LANES), 1) < LANES // 2

    def load_q(b):
        lat = jnp.concatenate(
            [jnp.concatenate([q_msg[g, b, t * lat_tiles + n] for n in range(lat_tiles)], axis=1)
             for g in range(group) for t in range(toks)], axis=0)
        rope = jnp.concatenate(
            [q_msg[g, b, toks * lat_tiles][:, t * ROPE:(t + 1) * ROPE]
             for g in range(group) for t in range(toks)], axis=0)
        return jnp.concatenate([lat, rope], axis=1)

    def scores(i, s, s_ref):
        slot = _mod(i, DEPTH)
        b = PAIR * i + s
        query = load_q(b)
        last = len_ref[b] - toks + row_tok
        best = None
        chunk = 512
        for n in range(seq_loc // chunk):
            at = pl.ds(n * chunk, chunk)
            sc = _nt_dot(query, kv_buf[slot, s, at, :])
            for t in range(chunk // tile):
                lo = n * chunk + t * tile
                piece = sc[:, t * tile:(t + 1) * tile] * scale2
                if lo + tile > always:
                    piece = jnp.where(col_pos[:, lo:lo + tile] <= last, piece, MASKED)
                s_ref[:, lo:lo + tile] = piece
                best = piece if best is None else jnp.maximum(best, piece)
        return jnp.max(best, axis=1, keepdims=True)

    def attend(i, s, s_ref, p_ref, top):
        slot, held = _mod(i, 2), _mod(i, DEPTH)
        total = None
        for n in range(seq_loc // tile):
            w = jnp.exp2(s_ref[:, n * tile:(n + 1) * tile] - top)
            total = w if total is None else total + w
            p_ref[:, n * tile:(n + 1) * tile] = w.astype(BF16)
        out = jnp.dot(p_ref[...], kv_buf[held, s, :, 0:LATENT], preferred_element_type=F32)
        norm = jnp.sum(total, axis=1, keepdims=True)
        stats = jnp.where(half[0:1], top, norm)
        h = group * rows // 2
        keep[slot, s, :, 0:LATENT] = out[:h]
        keep[slot, s, :, LATENT:LATENT + LANES] = stats[:h]
        part_send[slot, s, :, 0:LATENT] = out[h:]
        part_send[slot, s, :, LATENT:LATENT + LANES] = stats[h:]

    row_id = lax.broadcasted_iota(jnp.int32, (rows, LANES), 0)
    lane_id = lax.broadcasted_iota(jnp.int32, (rows, LANES), 1)

    def merge(i):
        slot = _mod(i, 2)
        lse_sum = None
        for s in range(PAIR):
            st_a = keep[slot, s, :, LATENT:LATENT + LANES]
            st_b = part_recv[i, s, :, LATENT:LATENT + LANES]
            m_a, l_a = st_a[:, 0:1], st_a[:, LANES // 2:LANES // 2 + 1]
            m_b, l_b = st_b[:, 0:1], st_b[:, LANES // 2:LANES // 2 + 1]
            m = jnp.maximum(m_a, m_b)
            w_a, w_b = jnp.exp2(m_a - m), jnp.exp2(m_b - m)
            norm = l_a * w_a + l_b * w_b
            lse = m + jnp.log2(norm)
            inv = 1.0 / norm
            both = keep[slot, s, :, 0:LATENT] * (w_a * inv) + part_recv[i, s, :, 0:LATENT] * (w_b * inv)
            mine[i, s] = both[:rows]
            ici_send[i, s] = both[rows:].astype(BF16)
            wide = jnp.broadcast_to(lse, (2 * rows, LANES))
            mine_lse[i, s] = wide[:rows]
            picked = jnp.where(lane_id == row_id + (s * rows + PAIR * rows * _mod(i, 2)), wide[rows:], 0.0)
            lse_sum = picked if lse_sum is None else lse_sum + picked
        k, r = lse_row(i)
        line = jnp.sum(lse_sum, axis=0, keepdims=True)
        before = lse_send[k, pl.ds(r, 1)]
        lse_send[k, pl.ds(r, 1)] = jnp.where(lane_id[0:1] // (PAIR * rows) == _mod(i, 2), line, before)

    def finish_weights(i):
        k, r = lse_row(i)
        row = jnp.broadcast_to(lse_recv[k, pl.ds(r, 1)], (rows, LANES))
        weights = []
        for s in range(PAIR):
            lane = row_id + (s * rows + PAIR * rows * _mod(i, 2))
            lse_b = jnp.sum(jnp.where(lane_id == lane, row, 0.0), axis=1, keepdims=True)
            lse_a = mine_lse[i, s, :, 0:1]
            m = jnp.maximum(lse_a, lse_b)
            w_a, w_b = jnp.exp2(lse_a - m), jnp.exp2(lse_b - m)
            inv = 1.0 / (w_a + w_b)
            weights.append((w_a * inv, w_b * inv))
        return weights

    def finish(i, weights=None):
        weights = finish_weights(i) if weights is None else weights
        for s in range(PAIR):
            o = mine[i, s] * weights[s][0] + ici_recv[i, s].astype(F32) * weights[s][1]
            out_buf[PAIR * i + s] = o.astype(BF16).reshape(toks, heads, LATENT)

    def when(i, phase, limit, action):
        if isinstance(i, int):
            if i % MSG == phase and i < limit:
                action()
        else:
            pl.when(jnp.logical_and(lax.rem(i, MSG) == phase, i < limit))(action)

    def step(i, compute=True, merging=True):
        if merging:
            part_copy(i - 2).wait()
        if not (isinstance(i, int) and i == 0):
            part_copy(i - 1).start()
        if compute:
            for s in range(PAIR):
                kv_copy(i, s).wait()

            def prefetch():
                for s in range(PAIR):
                    kv_copy(i + DEPTH - 1, s).start()

            def more():
                m = (i + AHEAD) // MSG + 3
                q_send(m, 1).start()
                q_send(m, 0).start()

            def forward(m):
                q_send(m, 1).wait_recv()
                q_send(m, 2).start()

            def arrived(m):
                q_send(m, 0).wait_recv()
                q_send(m, 2).wait_recv()

            if isinstance(i, int):
                if i + DEPTH - 1 < steps:
                    prefetch()
            else:
                pl.when(i + DEPTH - 1 < steps)(prefetch)
            when(i, 0, steps - AHEAD, more)
            if isinstance(i, int):
                if i < 2:
                    forward(i + 1)
                arrived(i)
            else:
                for m in (3, 4):
                    pl.when(i == heads_of[m][0] - 1)(functools.partial(forward, m))
                    pl.when(i == heads_of[m][0])(functools.partial(arrived, m))
                late = i > heads_of[4][0]
                pl.when(jnp.logical_and(late, jnp.logical_and(lax.rem(i, MSG) == MSG - 1, i < steps - 1)))(
                    lambda: forward((i + 1) // MSG + 3))
                pl.when(jnp.logical_and(late, lax.rem(i, MSG) == 0))(lambda: arrived(i // MSG + 3))
        if merging:
            merge(i - 2)
        if compute:
            tops = [scores(i, 0, s_a), scores(i, 1, s_b)]
            attend(i, 0, s_a, p_a, tops[0])
            attend(i, 1, s_b, p_b, tops[1])

    def send_out(i):
        k = (i - 2) // MSG - 1
        out_send(k).start()
        lse_send_copy(k).start()

    q_send(0, 1).wait_recv()
    q_send(0, 2).start()
    step(0, merging=False)
    step(1, merging=False)
    step(2)

    def body(i, carry):
        pl.when(jnp.logical_and(lax.rem(i, MSG) == 2, jnp.logical_and(i > MSG, i < steps - 4)))(lambda: send_out(i))
        pl.when(i == steps - 4)(out_send(long).start)

        @pl.when(i == steps - 2)
        def _():
            out_send(long + 1).start()
            lse_send_copy(long).start()

        step(i)
        return carry

    lax.fori_loop(3, steps, body, 0)
    out_send(long + 2).start()
    step(steps, compute=False)
    part_copy(steps - 1).wait()
    merge(steps - 1)
    lse_send_copy(groups - 1).start()
    out_send(long + 3).start()
    lse_send_copy(groups).start()
    out_send(long + 4).start()

    def q_sent(m, carry):
        for dest in range(3):
            q_send(m, dest).wait_send()
        return carry

    for m in range(5):
        q_sent(m, 0)
    lax.fori_loop(5, q_msgs, q_sent, 0)

    def tail(k, carry):
        out_send(k).wait()
        lse_send_copy(k).wait()
        for u in range(MSG):
            finish(MSG * k + u)
        return carry

    lax.fori_loop(0, long, tail, 0)
    out_send(long).wait()
    out_send(long + 1).wait()
    lse_send_copy(long).wait()
    for i in range(steps - 8, steps - 4):
        finish(i)
    out_send(long + 2).wait()
    lse_send_copy(groups - 1).wait()
    for i in range(steps - 4, steps - 2):
        finish(i)
    weights = finish_weights(steps - 2)
    out_send(long + 3).wait()
    finish(steps - 2, weights)
    lse_send_copy(groups).wait()
    weights = finish_weights(steps - 1)
    out_send(long + 4).wait()
    finish(steps - 1, weights)


def solution(mesh):
    def local_step(q_blk, kv_blk, len_blk):
        batch, toks, heads, width = q_blk.shape
        rounds = kv_blk.shape[1]
        seq_loc = rounds * PAGE
        steps = batch // PAIR
        rows = toks * heads
        keys = kv_blk.reshape(batch, seq_loc, width)
        wide = LATENT + LANES
        dma = pltpu.SemaphoreType.DMA
        return pl.pallas_call(
            _kernel,
            out_shape=pltpu.VMEM((batch, toks, heads, LATENT), BF16),
            in_specs=[
                pl.BlockSpec(memory_space=pl.ANY),
                pl.BlockSpec(memory_space=pl.ANY),
                pl.BlockSpec(memory_space=pl.ANY),
            ],
            out_specs=pl.BlockSpec(memory_space=pltpu.VMEM),
            scratch_shapes=[
                pltpu.SMEM((batch,), jnp.int32),
                pltpu.VMEM((batch, toks, heads, width), BF16),
                pltpu.VMEM((4, batch, toks * width // LANES, heads, LANES), BF16),
                pltpu.VMEM((DEPTH, PAIR, seq_loc, width), BF16),
                pltpu.VMEM((4 * rows, seq_loc), F32),
                pltpu.VMEM((4 * rows, seq_loc), F32),
                pltpu.VMEM((4 * rows, seq_loc), BF16),
                pltpu.VMEM((4 * rows, seq_loc), BF16),
                pltpu.VMEM((2, PAIR, 2 * rows, wide), F32),
                pltpu.VMEM((2, PAIR, 2 * rows, wide), F32),
                pltpu.VMEM((steps, PAIR, 2 * rows, wide), F32),
                pltpu.VMEM((steps, PAIR, rows, LATENT), F32),
                pltpu.VMEM((steps, PAIR, rows, LANES), F32),
                pltpu.VMEM((steps, PAIR, rows, LATENT), BF16),
                pltpu.VMEM((steps, PAIR, rows, LATENT), BF16),
                pltpu.VMEM((steps // MSG + 1, MSG // 2, LANES), F32),
                pltpu.VMEM((steps // MSG + 1, MSG // 2, LANES), F32),
                dma((4,)),
                dma((DEPTH, PAIR)),
                dma((3, steps // MSG + 3)),
                dma((3, steps // MSG + 3)),
                dma((2,)),
                dma((steps,)),
                dma((2, steps // MSG + 3)),
                dma((2, steps // MSG + 3)),
            ],
            compiler_params=pltpu.CompilerParams(
                collective_id=0, has_side_effects=True, vmem_limit_bytes=60_000_000),
            name='mla_decode',
        )(len_blk, q_blk, keys)

    return jax.shard_map(
        local_step, mesh=mesh,
        in_specs=(P('dp', None, 'dcp', None), P('dp', None, 'dcp', None, None), P('dp')),
        out_specs=P('dp', None, 'dcp', None), check_vma=False)
```

```python
import functools
import math

import jax
import jax.numpy as jnp
from jax import lax
from jax.experimental import pallas as pl
from jax.experimental.pallas import tpu as pltpu
from jax.sharding import PartitionSpec as P

LATENT = 512
ROPE = 64
NOPE = 128
PAGE = 64
MASKED = -math.inf
LANES = 128
PAIR = 2
FIRST = 2
AHEAD = 12
MSG = 4
DEPTH = 3
MESH_ID = pl.DeviceIdType.MESH
F32 = jnp.float32
BF16 = jnp.bfloat16


def _nt_dot(a, b):
    return lax.dot_general(a, b, (((1,), (1,)), ((), ())), preferred_element_type=F32)


def _mod(i, n):
    return i % n if isinstance(i, int) else lax.rem(i, n)


def _kernel(len_hbm, q_hbm, kv_hbm, out_buf,
            len_ref, q_own, q_msg, kv_buf, s_a, s_b, p_a, p_b,
            keep, part_send, part_recv, mine, mine_lse,
            ici_send, ici_recv, lse_send, lse_recv,
            own_sem, kv_sem, qs_sem, qr_sem, part_ssem, part_rsem, ici_ssem, ici_rsem):
    batch, toks, heads, width = q_own.shape
    steps = batch // PAIR
    seq_loc = kv_buf.shape[2]
    rows = toks * heads
    tile = LANES
    group = 4
    me = lax.axis_index('dcp')
    core = lax.rem(me, 2)
    partner = me + 1 - 2 * core
    across = lax.rem(me + 2, group)

    barrier = pltpu.get_barrier_semaphore()
    for peer in (partner, across):
        pl.semaphore_signal(barrier, inc=1, device_id={'dcp': peer}, device_id_type=MESH_ID)

    cuts = (0, PAIR * FIRST, PAIR * AHEAD, batch)
    own_copies = []
    for k in range(3):
        at = pl.ds(cuts[k], cuts[k + 1] - cuts[k])
        own_copies.append(pltpu.make_async_copy(q_hbm.at[at], q_own.at[at], own_sem.at[k]))
        own_copies[-1].start()

    len_copy = pltpu.make_async_copy(len_hbm, len_ref, own_sem.at[3])
    len_copy.start()

    def kv_copy(i, s):
        slot = _mod(i, DEPTH)
        return pltpu.make_async_copy(kv_hbm.at[PAIR * i + s], kv_buf.at[slot, s], kv_sem.at[slot, s])

    def pair(i):
        return pl.ds(PAIR * i, PAIR)

    heads_of = ((0, 1), (1, 1), (2, 2), (4, 2), (6, 2))
    q_msgs = steps // MSG + 3

    def q_send(m, dest):
        slot = (2, 1, 3)[dest]
        first, count = heads_of[m] if isinstance(m, int) and m < 5 else (MSG * (m - 3), MSG)
        at = pl.ds(PAIR * first, PAIR * count)
        return pltpu.make_async_remote_copy(
            src_ref=q_msg.at[1 if dest == 2 else 0, at], dst_ref=q_msg.at[slot, at],
            send_sem=qs_sem.at[dest, m], recv_sem=qr_sem.at[slot - 1, m],
            device_id={'dcp': (partner, across, partner)[dest]}, device_id_type=MESH_ID)

    def part_copy(i):
        slot = _mod(i, 2)
        return pltpu.make_async_remote_copy(
            src_ref=part_send.at[slot], dst_ref=part_recv.at[i],
            send_sem=part_ssem.at[slot], recv_sem=part_rsem.at[i],
            device_id={'dcp': partner}, device_id_type=MESH_ID)

    out_parts = ((0, 8), (8, 8), (16, 4), (20, 4), (24, 2), (26, 2), (28, 2), (30, 1), (31, 1))
    lse_parts = ((0, 4), (4, 4), (8, 2), (10, 2), (12, 2), (14, 2), (16, 1))

    def across_copy(src, dst, at, kind, m):
        return pltpu.make_async_remote_copy(
            src_ref=src.at[at], dst_ref=dst.at[at],
            send_sem=ici_ssem.at[kind, m], recv_sem=ici_rsem.at[kind, m],
            device_id={'dcp': across}, device_id_type=MESH_ID)

    def out_send(m):
        return across_copy(ici_send, ici_recv, pl.ds(*out_parts[m]), 0, m)

    def lse_send_copy(m):
        return across_copy(lse_send, lse_recv, pl.ds(*lse_parts[m]), 1, m)

    def lse_row(i):
        return steps // 2 if isinstance(i, int) and i == steps - 1 else i // 2

    unroll = PAIR * FIRST
    lat_tiles = LATENT // LANES

    def pack(k, carry):
        for u in range(unroll):
            b = unroll * k + u
            for t in range(toks):
                for n in range(lat_tiles):
                    q_msg[0, b, t * lat_tiles + n] = q_own[b, t, :, n * LANES:(n + 1) * LANES]
            q_msg[0, b, toks * lat_tiles] = jnp.concatenate(
                [q_own[b, t, :, LATENT:width] for t in range(toks)], axis=-1)
        return carry

    own_copies[0].wait()
    pack(0, 0)
    pl.semaphore_wait(barrier, 2)
    for k in range(2):
        if k == 1:
            own_copies[1].wait()
            lax.fori_loop(1, cuts[2] // unroll, pack, 0)
        for m in ((0, 1), range(2, AHEAD // MSG + 3))[k]:
            q_send(m, 1).start()
            q_send(m, 0).start()
    for i in range(DEPTH - 1):
        for s in range(PAIR):
            kv_copy(i, s).start()
    len_copy.wait()
    own_copies[2].wait()
    lax.fori_loop(cuts[2] // unroll, batch // unroll, pack, 0)

    scale2 = (NOPE + ROPE) ** -0.5 * math.log2(math.e)
    row_tok = lax.rem(lax.broadcasted_iota(jnp.int32, (group * rows, 1), 0) // heads, toks)
    col = lax.broadcasted_iota(jnp.int32, (1, seq_loc), 1)
    col_pos = (col // PAGE) * (group * PAGE) + lax.rem(col, PAGE) + me * PAGE
    always = seq_loc // 2 - PAGE
    half = lax.broadcasted_iota(jnp.int32, (group * rows // 2, LANES), 1) < LANES // 2

    def load_q(b):
        lat = jnp.concatenate(
            [jnp.concatenate([q_msg[g, b, t * lat_tiles + n] for n in range(lat_tiles)], axis=1)
             for g in range(group) for t in range(toks)], axis=0)
        rope = jnp.concatenate(
            [q_msg[g, b, toks * lat_tiles][:, t * ROPE:(t + 1) * ROPE]
             for g in range(group) for t in range(toks)], axis=0)
        return jnp.concatenate([lat, rope], axis=1)

    def scores(i, s, s_ref):
        slot = _mod(i, DEPTH)
        b = PAIR * i + s
        query = load_q(b)
        last = len_ref[b] - toks + row_tok
        best = None
        chunk = 512
        for n in range(seq_loc // chunk):
            at = pl.ds(n * chunk, chunk)
            sc = _nt_dot(query, kv_buf[slot, s, at, :])
            for t in range(chunk // tile):
                lo = n * chunk + t * tile
                piece = sc[:, t * tile:(t + 1) * tile] * scale2
                if lo + tile > always:
                    piece = jnp.where(col_pos[:, lo:lo + tile] <= last, piece, MASKED)
                s_ref[:, lo:lo + tile] = piece
                best = piece if best is None else jnp.maximum(best, piece)
        return jnp.max(best, axis=1, keepdims=True)

    def attend(i, s, s_ref, p_ref, top):
        slot, held = _mod(i, 2), _mod(i, DEPTH)
        total = None
        for n in range(seq_loc // tile):
            w = jnp.exp2(s_ref[:, n * tile:(n + 1) * tile] - top)
            total = w if total is None else total + w
            p_ref[:, n * tile:(n + 1) * tile] = w.astype(BF16)
        out = jnp.dot(p_ref[...], kv_buf[held, s, :, 0:LATENT], preferred_element_type=F32)
        norm = jnp.sum(total, axis=1, keepdims=True)
        stats = jnp.where(half[0:1], top, norm)
        h = group * rows // 2
        keep[slot, s, :, 0:LATENT] = out[:h]
        keep[slot, s, :, LATENT:LATENT + LANES] = stats[:h]
        part_send[slot, s, :, 0:LATENT] = out[h:]
        part_send[slot, s, :, LATENT:LATENT + LANES] = stats[h:]

    row_id = lax.broadcasted_iota(jnp.int32, (rows, LANES), 0)
    lane_id = lax.broadcasted_iota(jnp.int32, (rows, LANES), 1)

    def merge(i):
        slot = _mod(i, 2)
        lse_sum = None
        for s in range(PAIR):
            st_a = keep[slot, s, :, LATENT:LATENT + LANES]
            st_b = part_recv[i, s, :, LATENT:LATENT + LANES]
            m_a, l_a = st_a[:, 0:1], st_a[:, LANES // 2:LANES // 2 + 1]
            m_b, l_b = st_b[:, 0:1], st_b[:, LANES // 2:LANES // 2 + 1]
            m = jnp.maximum(m_a, m_b)
            w_a, w_b = jnp.exp2(m_a - m), jnp.exp2(m_b - m)
            norm = l_a * w_a + l_b * w_b
            lse = m + jnp.log2(norm)
            inv = 1.0 / norm
            both = keep[slot, s, :, 0:LATENT] * (w_a * inv) + part_recv[i, s, :, 0:LATENT] * (w_b * inv)
            mine[i, s] = both[:rows]
            ici_send[i, s] = both[rows:].astype(BF16)
            wide = jnp.broadcast_to(lse, (2 * rows, LANES))
            mine_lse[i, s] = wide[:rows]
            picked = jnp.where(lane_id == row_id + (s * rows + PAIR * rows * _mod(i, 2)), wide[rows:], 0.0)
            lse_sum = picked if lse_sum is None else lse_sum + picked
        line = jnp.sum(lse_sum, axis=0, keepdims=True)
        before = lse_send[lse_row(i)]
        lse_send[lse_row(i)] = jnp.where(lane_id[0:1] // (PAIR * rows) == _mod(i, 2), line, before)

    def finish_weights(i):
        row = jnp.broadcast_to(lse_recv[lse_row(i)], (rows, LANES))
        weights = []
        for s in range(PAIR):
            lane = row_id + (s * rows + PAIR * rows * _mod(i, 2))
            lse_b = jnp.sum(jnp.where(lane_id == lane, row, 0.0), axis=1, keepdims=True)
            lse_a = mine_lse[i, s, :, 0:1]
            m = jnp.maximum(lse_a, lse_b)
            w_a, w_b = jnp.exp2(lse_a - m), jnp.exp2(lse_b - m)
            inv = 1.0 / (w_a + w_b)
            weights.append((w_a * inv, w_b * inv))
        return weights

    def finish(i, weights=None):
        weights = finish_weights(i) if weights is None else weights
        for s in range(PAIR):
            o = mine[i, s] * weights[s][0] + ici_recv[i, s].astype(F32) * weights[s][1]
            out_buf[PAIR * i + s] = o.astype(BF16).reshape(toks, heads, LATENT)

    def when(i, phase, limit, action):
        if isinstance(i, int):
            if i % MSG == phase and i < limit:
                action()
        else:
            pl.when(jnp.logical_and(lax.rem(i, MSG) == phase, i < limit))(action)

    def step(i, compute=True, merging=True):
        if merging:
            part_copy(i - 2).wait()
        if not (isinstance(i, int) and i == 0):
            part_copy(i - 1).start()
        if compute:
            for s in range(PAIR):
                kv_copy(i, s).wait()

            def prefetch():
                for s in range(PAIR):
                    kv_copy(i + DEPTH - 1, s).start()

            def more():
                m = (i + AHEAD) // MSG + 3
                q_send(m, 1).start()
                q_send(m, 0).start()

            def forward(m):
                q_send(m, 1).wait_recv()
                q_send(m, 2).start()

            def arrived(m):
                q_send(m, 0).wait_recv()
                q_send(m, 2).wait_recv()

            if isinstance(i, int):
                if i + DEPTH - 1 < steps:
                    prefetch()
            else:
                pl.when(i + DEPTH - 1 < steps)(prefetch)
            when(i, 0, steps - AHEAD, more)
            if isinstance(i, int):
                if i < 2:
                    forward(i + 1)
                arrived(i)
            else:
                for m in range(3, 5):
                    pl.when(i == heads_of[m][0] - 1)(functools.partial(forward, m))
                    pl.when(i == heads_of[m][0])(functools.partial(arrived, m))
                late = i > heads_of[4][0]
                pl.when(jnp.logical_and(late, jnp.logical_and(lax.rem(i, MSG) == MSG - 1, i < steps - 1)))(
                    lambda: forward((i + 1) // MSG + 3))
                pl.when(jnp.logical_and(late, lax.rem(i, MSG) == 0))(lambda: arrived(i // MSG + 3))
        if merging:
            merge(i - 2)
        if compute:
            tops = [scores(i, 0, s_a), scores(i, 1, s_b)]
            attend(i, 0, s_a, p_a, tops[0])
            attend(i, 1, s_b, p_b, tops[1])

    q_send(0, 1).wait_recv()
    q_send(0, 2).start()
    step(0, merging=False)
    step(1, merging=False)
    step(2)

    def body(i, carry):
        for m in range(6):
            @pl.when(i == sum(out_parts[m]) + 2)
            def _():
                out_send(m).start()
                if m != 4:
                    lse_send_copy(m if m < 4 else 4).start()

        step(i)
        return carry

    lax.fori_loop(3, steps, body, 0)
    out_send(6).start()
    step(steps, compute=False)
    part_copy(steps - 1).wait()
    merge(steps - 1)
    lse_send_copy(5).start()
    out_send(7).start()
    lse_send_copy(6).start()
    out_send(8).start()

    def q_sent(m, carry):
        for dest in range(3):
            q_send(m, dest).wait_send()
        return carry

    for m in range(5):
        q_sent(m, 0)
    lax.fori_loop(5, q_msgs, q_sent, 0)

    def tail(k, carry):
        for u in range(4):
            finish(4 * k + u)
        return carry

    for m in range(4):
        out_send(m).wait()
        lse_send_copy(m).wait()
        first, count = out_parts[m]
        lax.fori_loop(first // 4, (first + count) // 4, tail, 0)
    out_send(4).wait()
    out_send(5).wait()
    lse_send_copy(4).wait()
    tail(6, 0)
    out_send(6).wait()
    lse_send_copy(5).wait()
    finish(steps - 4)
    finish(steps - 3)
    weights = finish_weights(steps - 2)
    out_send(7).wait()
    finish(steps - 2, weights)
    lse_send_copy(6).wait()
    weights = finish_weights(steps - 1)
    out_send(8).wait()
    finish(steps - 1, weights)


def solution(mesh):
    def local_step(q_blk, kv_blk, len_blk):
        batch, toks, heads, width = q_blk.shape
        rounds = kv_blk.shape[1]
        seq_loc = rounds * PAGE
        steps = batch // PAIR
        rows = toks * heads
        keys = kv_blk.reshape(batch, seq_loc, width)
        wide = LATENT + LANES
        dma = pltpu.SemaphoreType.DMA
        return pl.pallas_call(
            _kernel,
            out_shape=pltpu.VMEM((batch, toks, heads, LATENT), BF16),
            in_specs=[
                pl.BlockSpec(memory_space=pl.ANY),
                pl.BlockSpec(memory_space=pl.ANY),
                pl.BlockSpec(memory_space=pl.ANY),
            ],
            out_specs=pl.BlockSpec(memory_space=pltpu.VMEM),
            scratch_shapes=[
                pltpu.SMEM((batch,), jnp.int32),
                pltpu.VMEM((batch, toks, heads, width), BF16),
                pltpu.VMEM((4, batch, toks * width // LANES, heads, LANES), BF16),
                pltpu.VMEM((DEPTH, PAIR, seq_loc, width), BF16),
                pltpu.VMEM((4 * rows, seq_loc), F32),
                pltpu.VMEM((4 * rows, seq_loc), F32),
                pltpu.VMEM((4 * rows, seq_loc), BF16),
                pltpu.VMEM((4 * rows, seq_loc), BF16),
                pltpu.VMEM((2, PAIR, 2 * rows, wide), F32),
                pltpu.VMEM((2, PAIR, 2 * rows, wide), F32),
                pltpu.VMEM((steps, PAIR, 2 * rows, wide), F32),
                pltpu.VMEM((steps, PAIR, rows, LATENT), F32),
                pltpu.VMEM((steps, PAIR, rows, LANES), F32),
                pltpu.VMEM((steps, PAIR, rows, LATENT), BF16),
                pltpu.VMEM((steps, PAIR, rows, LATENT), BF16),
                pltpu.VMEM((steps // 2 + 1, 1, LANES), F32),
                pltpu.VMEM((steps // 2 + 1, 1, LANES), F32),
                dma((4,)),
                dma((DEPTH, PAIR)),
                dma((3, steps // MSG + 3)),
                dma((3, steps // MSG + 3)),
                dma((2,)),
                dma((steps,)),
                dma((2, 9)),
                dma((2, 9)),
            ],
            compiler_params=pltpu.CompilerParams(
                collective_id=0, has_side_effects=True, vmem_limit_bytes=60_000_000),
            name='mla_decode',
        )(len_blk, q_blk, keys)

    return jax.shard_map(
        local_step, mesh=mesh,
        in_specs=(P('dp', None, 'dcp', None), P('dp', None, 'dcp', None, None), P('dp')),
        out_specs=P('dp', None, 'dcp', None), check_vma=False)
```

```python
import functools
import math

import jax
import jax.numpy as jnp
from jax import lax
from jax.experimental import pallas as pl
from jax.experimental.pallas import tpu as pltpu
from jax.sharding import PartitionSpec as P

LATENT = 512
ROPE = 64
NOPE = 128
PAGE = 64
MASKED = -math.inf
LANES = 128
PAIR = 2
FIRST = 2
AHEAD = 12
MSG = 4
DEPTH = 3
MESH_ID = pl.DeviceIdType.MESH
F32 = jnp.float32
BF16 = jnp.bfloat16


def _nt_dot(a, b):
    return lax.dot_general(a, b, (((1,), (1,)), ((), ())), preferred_element_type=F32)


def _mod(i, n):
    return i % n if isinstance(i, int) else lax.rem(i, n)


def _kernel(len_hbm, q_hbm, kv_hbm, out_buf,
            len_ref, q_own, q_msg, kv_buf, s_a, s_b, p_a, p_b,
            keep, part_send, part_recv, mine, mine_lse,
            ici_send, ici_recv, lse_send, lse_recv,
            own_sem, kv_sem, qs_sem, qr_sem, part_ssem, part_rsem, ici_ssem, ici_rsem):
    batch, toks, heads, width = q_own.shape
    steps = batch // PAIR
    seq_loc = kv_buf.shape[2]
    rows = toks * heads
    tile = LANES
    group = 4
    me = lax.axis_index('dcp')
    core = lax.rem(me, 2)
    partner = me + 1 - 2 * core
    across = lax.rem(me + 2, group)

    barrier = pltpu.get_barrier_semaphore()
    for peer in (partner, across):
        pl.semaphore_signal(barrier, inc=1, device_id={'dcp': peer}, device_id_type=MESH_ID)

    cuts = (0, PAIR * FIRST, PAIR * AHEAD, batch)
    own_copies = []
    for k in range(3):
        at = pl.ds(cuts[k], cuts[k + 1] - cuts[k])
        own_copies.append(pltpu.make_async_copy(q_hbm.at[at], q_own.at[at], own_sem.at[k]))
        own_copies[-1].start()

    len_copy = pltpu.make_async_copy(len_hbm, len_ref, own_sem.at[3])
    len_copy.start()

    def kv_copy(i, s):
        slot = _mod(i, DEPTH)
        return pltpu.make_async_copy(kv_hbm.at[PAIR * i + s], kv_buf.at[slot, s], kv_sem.at[slot, s])

    def pair(i):
        return pl.ds(PAIR * i, PAIR)

    heads_of = ((0, 1), (1, 1), (2, 2), (4, 2), (6, 2))
    q_msgs = steps // MSG + 3

    def q_send(m, dest):
        slot = (2, 1, 3)[dest]
        first, count = heads_of[m] if isinstance(m, int) and m < 5 else (MSG * (m - 3), MSG)
        at = pl.ds(PAIR * first, PAIR * count)
        return pltpu.make_async_remote_copy(
            src_ref=q_msg.at[1 if dest == 2 else 0, at], dst_ref=q_msg.at[slot, at],
            send_sem=qs_sem.at[dest, m], recv_sem=qr_sem.at[slot - 1, m],
            device_id={'dcp': (partner, across, partner)[dest]}, device_id_type=MESH_ID)

    def part_copy(i):
        slot = _mod(i, 2)
        return pltpu.make_async_remote_copy(
            src_ref=part_send.at[slot], dst_ref=part_recv.at[i],
            send_sem=part_ssem.at[slot], recv_sem=part_rsem.at[i],
            device_id={'dcp': partner}, device_id_type=MESH_ID)

    out_parts = ((0, 8), (8, 8), (16, 4), (20, 4), (24, 4), (28, 2), (30, 1), (31, 1))
    lse_parts = ((0, 4), (4, 4), (8, 2), (10, 2), (12, 2), (14, 2), (16, 1))

    def across_copy(src, dst, at, kind, m):
        return pltpu.make_async_remote_copy(
            src_ref=src.at[at], dst_ref=dst.at[at],
            send_sem=ici_ssem.at[kind, m], recv_sem=ici_rsem.at[kind, m],
            device_id={'dcp': across}, device_id_type=MESH_ID)

    def out_send(m):
        return across_copy(ici_send, ici_recv, pl.ds(*out_parts[m]), 0, m)

    def lse_send_copy(m):
        return across_copy(lse_send, lse_recv, pl.ds(*lse_parts[m]), 1, m)

    def lse_row(i):
        return steps // 2 if isinstance(i, int) and i == steps - 1 else i // 2

    unroll = PAIR * FIRST
    lat_tiles = LATENT // LANES

    def pack(k, carry):
        for u in range(unroll):
            b = unroll * k + u
            for t in range(toks):
                for n in range(lat_tiles):
                    q_msg[0, b, t * lat_tiles + n] = q_own[b, t, :, n * LANES:(n + 1) * LANES]
            q_msg[0, b, toks * lat_tiles] = jnp.concatenate(
                [q_own[b, t, :, LATENT:width] for t in range(toks)], axis=-1)
        return carry

    own_copies[0].wait()
    pack(0, 0)
    pl.semaphore_wait(barrier, 2)
    for k in range(2):
        if k == 1:
            own_copies[1].wait()
            lax.fori_loop(1, cuts[2] // unroll, pack, 0)
        for m in ((0, 1), range(2, AHEAD // MSG + 3))[k]:
            q_send(m, 1).start()
            q_send(m, 0).start()
    for i in range(DEPTH - 1):
        for s in range(PAIR):
            kv_copy(i, s).start()
    len_copy.wait()
    own_copies[2].wait()
    lax.fori_loop(cuts[2] // unroll, batch // unroll, pack, 0)

    scale2 = (NOPE + ROPE) ** -0.5 * math.log2(math.e)
    row_tok = lax.rem(lax.broadcasted_iota(jnp.int32, (group * rows, 1), 0) // heads, toks)
    col = lax.broadcasted_iota(jnp.int32, (1, seq_loc), 1)
    col_pos = (col // PAGE) * (group * PAGE) + lax.rem(col, PAGE) + me * PAGE
    always = seq_loc // 2 - PAGE
    half = lax.broadcasted_iota(jnp.int32, (group * rows // 2, LANES), 1) < LANES // 2

    def load_q(b):
        lat = jnp.concatenate(
            [jnp.concatenate([q_msg[g, b, t * lat_tiles + n] for n in range(lat_tiles)], axis=1)
             for g in range(group) for t in range(toks)], axis=0)
        rope = jnp.concatenate(
            [q_msg[g, b, toks * lat_tiles][:, t * ROPE:(t + 1) * ROPE]
             for g in range(group) for t in range(toks)], axis=0)
        return jnp.concatenate([lat, rope], axis=1)

    def scores(i, s, s_ref):
        slot = _mod(i, DEPTH)
        b = PAIR * i + s
        query = load_q(b)
        last = len_ref[b] - toks + row_tok
        best = None
        chunk = 512
        for n in range(seq_loc // chunk):
            at = pl.ds(n * chunk, chunk)
            sc = _nt_dot(query, kv_buf[slot, s, at, :])
            for t in range(chunk // tile):
                lo = n * chunk + t * tile
                piece = sc[:, t * tile:(t + 1) * tile] * scale2
                if lo + tile > always:
                    piece = jnp.where(col_pos[:, lo:lo + tile] <= last, piece, MASKED)
                s_ref[:, lo:lo + tile] = piece
                best = piece if best is None else jnp.maximum(best, piece)
        return jnp.max(best, axis=1, keepdims=True)

    def attend(i, s, s_ref, p_ref, top):
        slot, held = _mod(i, 2), _mod(i, DEPTH)
        total = None
        for n in range(seq_loc // tile):
            w = jnp.exp2(s_ref[:, n * tile:(n + 1) * tile] - top)
            total = w if total is None else total + w
            p_ref[:, n * tile:(n + 1) * tile] = w.astype(BF16)
        out = jnp.dot(p_ref[...], kv_buf[held, s, :, 0:LATENT], preferred_element_type=F32)
        norm = jnp.sum(total, axis=1, keepdims=True)
        stats = jnp.where(half[0:1], top, norm)
        h = group * rows // 2
        keep[slot, s, :, 0:LATENT] = out[:h]
        keep[slot, s, :, LATENT:LATENT + LANES] = stats[:h]
        part_send[slot, s, :, 0:LATENT] = out[h:]
        part_send[slot, s, :, LATENT:LATENT + LANES] = stats[h:]

    row_id = lax.broadcasted_iota(jnp.int32, (rows, LANES), 0)
    lane_id = lax.broadcasted_iota(jnp.int32, (rows, LANES), 1)

    def merge(i):
        slot = _mod(i, 2)
        lse_sum = None
        for s in range(PAIR):
            st_a = keep[slot, s, :, LATENT:LATENT + LANES]
            st_b = part_recv[i, s, :, LATENT:LATENT + LANES]
            m_a, l_a = st_a[:, 0:1], st_a[:, LANES // 2:LANES // 2 + 1]
            m_b, l_b = st_b[:, 0:1], st_b[:, LANES // 2:LANES // 2 + 1]
            m = jnp.maximum(m_a, m_b)
            w_a, w_b = jnp.exp2(m_a - m), jnp.exp2(m_b - m)
            norm = l_a * w_a + l_b * w_b
            lse = m + jnp.log2(norm)
            inv = 1.0 / norm
            both = keep[slot, s, :, 0:LATENT] * (w_a * inv) + part_recv[i, s, :, 0:LATENT] * (w_b * inv)
            mine[i, s] = both[:rows]
            ici_send[i, s] = both[rows:].astype(BF16)
            wide = jnp.broadcast_to(lse, (2 * rows, LANES))
            mine_lse[i, s] = wide[:rows]
            picked = jnp.where(lane_id == row_id + (s * rows + PAIR * rows * _mod(i, 2)), wide[rows:], 0.0)
            lse_sum = picked if lse_sum is None else lse_sum + picked
        line = jnp.sum(lse_sum, axis=0, keepdims=True)
        before = lse_send[lse_row(i)]
        lse_send[lse_row(i)] = jnp.where(lane_id[0:1] // (PAIR * rows) == _mod(i, 2), line, before)

    def finish_weights(i):
        row = jnp.broadcast_to(lse_recv[lse_row(i)], (rows, LANES))
        weights = []
        for s in range(PAIR):
            lane = row_id + (s * rows + PAIR * rows * _mod(i, 2))
            lse_b = jnp.sum(jnp.where(lane_id == lane, row, 0.0), axis=1, keepdims=True)
            lse_a = mine_lse[i, s, :, 0:1]
            m = jnp.maximum(lse_a, lse_b)
            w_a, w_b = jnp.exp2(lse_a - m), jnp.exp2(lse_b - m)
            inv = 1.0 / (w_a + w_b)
            weights.append((w_a * inv, w_b * inv))
        return weights

    def finish(i, weights=None):
        weights = finish_weights(i) if weights is None else weights
        for s in range(PAIR):
            o = mine[i, s] * weights[s][0] + ici_recv[i, s].astype(F32) * weights[s][1]
            out_buf[PAIR * i + s] = o.astype(BF16).reshape(toks, heads, LATENT)

    def when(i, phase, limit, action):
        if isinstance(i, int):
            if i % MSG == phase and i < limit:
                action()
        else:
            pl.when(jnp.logical_and(lax.rem(i, MSG) == phase, i < limit))(action)

    def step(i, compute=True, merging=True):
        if merging:
            part_copy(i - 2).wait()
        if not (isinstance(i, int) and i == 0):
            part_copy(i - 1).start()
        if compute:
            for s in range(PAIR):
                kv_copy(i, s).wait()

            def prefetch():
                for s in range(PAIR):
                    kv_copy(i + DEPTH - 1, s).start()

            def more():
                m = (i + AHEAD) // MSG + 3
                q_send(m, 1).start()
                q_send(m, 0).start()

            def forward(m):
                q_send(m, 1).wait_recv()
                q_send(m, 2).start()

            def arrived(m):
                q_send(m, 0).wait_recv()
                q_send(m, 2).wait_recv()

            if isinstance(i, int):
                if i + DEPTH - 1 < steps:
                    prefetch()
            else:
                pl.when(i + DEPTH - 1 < steps)(prefetch)
            when(i, 0, steps - AHEAD, more)
            if isinstance(i, int):
                if i < 2:
                    forward(i + 1)
                arrived(i)
            else:
                for m in range(3, 5):
                    pl.when(i == heads_of[m][0] - 1)(functools.partial(forward, m))
                    pl.when(i == heads_of[m][0])(functools.partial(arrived, m))
                late = i > heads_of[4][0]
                pl.when(jnp.logical_and(late, jnp.logical_and(lax.rem(i, MSG) == MSG - 1, i < steps - 1)))(
                    lambda: forward((i + 1) // MSG + 3))
                pl.when(jnp.logical_and(late, lax.rem(i, MSG) == 0))(lambda: arrived(i // MSG + 3))
        if merging:
            merge(i - 2)
        if compute:
            tops = [scores(i, 0, s_a), scores(i, 1, s_b)]
            attend(i, 0, s_a, p_a, tops[0])
            attend(i, 1, s_b, p_b, tops[1])

    q_send(0, 1).wait_recv()
    q_send(0, 2).start()
    step(0, merging=False)
    step(1, merging=False)
    step(2)

    def body(i, carry):
        for m in range(5):
            @pl.when(i == sum(out_parts[m]) + 2)
            def _():
                out_send(m).start()
                lse_send_copy(m).start()

        step(i)
        return carry

    lax.fori_loop(3, steps, body, 0)
    out_send(5).start()
    step(steps, compute=False)
    part_copy(steps - 1).wait()
    merge(steps - 1)
    lse_send_copy(5).start()
    out_send(6).start()
    lse_send_copy(6).start()
    out_send(7).start()

    def q_sent(m, carry):
        for dest in range(3):
            q_send(m, dest).wait_send()
        return carry

    for m in range(5):
        q_sent(m, 0)
    lax.fori_loop(5, q_msgs, q_sent, 0)

    def tail(k, carry):
        for u in range(4):
            finish(4 * k + u)
        return carry

    for m in range(4):
        out_send(m).wait()
        lse_send_copy(m).wait()
        first, count = out_parts[m]
        lax.fori_loop(first // 4, (first + count) // 4, tail, 0)
    out_send(4).wait()
    lse_send_copy(4).wait()
    tail(6, 0)
    out_send(5).wait()
    lse_send_copy(5).wait()
    finish(steps - 4)
    finish(steps - 3)
    weights = finish_weights(steps - 2)
    out_send(6).wait()
    finish(steps - 2, weights)
    lse_send_copy(6).wait()
    weights = finish_weights(steps - 1)
    out_send(7).wait()
    finish(steps - 1, weights)


def solution(mesh):
    def local_step(q_blk, kv_blk, len_blk):
        batch, toks, heads, width = q_blk.shape
        rounds = kv_blk.shape[1]
        seq_loc = rounds * PAGE
        steps = batch // PAIR
        rows = toks * heads
        keys = kv_blk.reshape(batch, seq_loc, width)
        wide = LATENT + LANES
        dma = pltpu.SemaphoreType.DMA
        return pl.pallas_call(
            _kernel,
            out_shape=pltpu.VMEM((batch, toks, heads, LATENT), BF16),
            in_specs=[
                pl.BlockSpec(memory_space=pl.ANY),
                pl.BlockSpec(memory_space=pl.ANY),
                pl.BlockSpec(memory_space=pl.ANY),
            ],
            out_specs=pl.BlockSpec(memory_space=pltpu.VMEM),
            scratch_shapes=[
                pltpu.SMEM((batch,), jnp.int32),
                pltpu.VMEM((batch, toks, heads, width), BF16),
                pltpu.VMEM((4, batch, toks * width // LANES, heads, LANES), BF16),
                pltpu.VMEM((DEPTH, PAIR, seq_loc, width), BF16),
                pltpu.VMEM((4 * rows, seq_loc), F32),
                pltpu.VMEM((4 * rows, seq_loc), F32),
                pltpu.VMEM((4 * rows, seq_loc), BF16),
                pltpu.VMEM((4 * rows, seq_loc), BF16),
                pltpu.VMEM((2, PAIR, 2 * rows, wide), F32),
                pltpu.VMEM((2, PAIR, 2 * rows, wide), F32),
                pltpu.VMEM((steps, PAIR, 2 * rows, wide), F32),
                pltpu.VMEM((steps, PAIR, rows, LATENT), F32),
                pltpu.VMEM((steps, PAIR, rows, LANES), F32),
                pltpu.VMEM((steps, PAIR, rows, LATENT), BF16),
                pltpu.VMEM((steps, PAIR, rows, LATENT), BF16),
                pltpu.VMEM((steps // 2 + 1, 1, LANES), F32),
                pltpu.VMEM((steps // 2 + 1, 1, LANES), F32),
                dma((4,)),
                dma((DEPTH, PAIR)),
                dma((3, steps // MSG + 3)),
                dma((3, steps // MSG + 3)),
                dma((2,)),
                dma((steps,)),
                dma((2, 8)),
                dma((2, 8)),
            ],
            compiler_params=pltpu.CompilerParams(
                collective_id=0, has_side_effects=True, vmem_limit_bytes=60_000_000),
            name='mla_decode',
        )(len_blk, q_blk, keys)

    return jax.shard_map(
        local_step, mesh=mesh,
        in_specs=(P('dp', None, 'dcp', None), P('dp', None, 'dcp', None, None), P('dp')),
        out_specs=P('dp', None, 'dcp', None), check_vma=False)
```
